32 devices in a mesh: dp: 4 (over y, z), tp: 8 (over x, core).
Axes of the slice: x: 4, y: 2, z: 2, core: 2. Of those that a mesh axis runs over, the one named last changes fastest.
The devices are a block of a 4x4x8 slice.
Arguments:
- x: bfloat16 [16, 1536, 3584], P('dp'), parts along dimension 0
- gamma: float32 [3584], replicated
- beta: float32 [3584], replicated
- wq: bfloat16 [3584, 4096], P(None, 'tp')
- wkv: bfloat16 [3584, 512], replicated
- wo: bfloat16 [4096, 3584], P('tp')
- w1: bfloat16 [3584, 14336], P(None, 'tp')
- w3: bfloat16 [3584, 14336], P(None, 'tp')
- w2: bfloat16 [14336, 3584], P('tp')
Outputs:
- output: bfloat16 [16, 1536, 3584], P('dp'), parts along dimension 0
There are 4 independent parts. The reference program is written for one: setup_inputs(seed, part) draws one part's arguments, and reference() takes and returns one part's arrays. A program takes and returns all parts, laid end to end along the dimension named above; an argument that names none is the same for every part.
All inputs are finite; a program needn't handle non-finite values.
Results may differ from the reference program's by a relative error of at most 0.0125769.
Values are sent between devices in bfloat16 or wider.
A program may use at most 768 MiB of HBM per device.

```python
import jax
import jax.numpy as jnp
from jax import lax
import math

D = 3584
HEADS = 16
HEAD = 256
FF = 14336
BATCH = 4
SEQ = 1536
EPS = 1e-5


def setup_inputs(seed: int = 0, part: int = 0) -> dict:
    key = jax.random.key(seed)
    ks = jax.random.split(key, 8)
    kx = jax.random.fold_in(jax.random.key(seed + 1), part)
    qscale = 0.85 * math.sqrt(max(1.0, math.log(SEQ / 32.0))) * D ** -0.5
    x = jax.random.normal(kx, (BATCH, SEQ, D), jnp.float32).astype(jnp.bfloat16)
    gamma = 1.0 + 0.3 * jax.random.normal(ks[0], (D,), jnp.float32)
    beta = 0.3 * jax.random.normal(ks[1], (D,), jnp.float32)
    wq = (qscale * jax.random.normal(ks[2], (D, HEADS * HEAD), jnp.float32)).astype(jnp.bfloat16)
    wkv = (D ** -0.5 * jax.random.normal(ks[3], (D, 2 * HEAD), jnp.float32)).astype(jnp.bfloat16)
    wo = (3.0 * (HEADS * HEAD) ** -0.5 * jax.random.normal(ks[4], (HEADS * HEAD, D), jnp.float32)).astype(jnp.bfloat16)
    w1 = (D ** -0.5 * jax.random.normal(ks[5], (D, FF), jnp.float32)).astype(jnp.bfloat16)
    w3 = (D ** -0.5 * jax.random.normal(ks[6], (D, FF), jnp.float32)).astype(jnp.bfloat16)
    w2 = (1.5 * FF ** -0.5 * jax.random.normal(ks[7], (FF, D), jnp.float32)).astype(jnp.bfloat16)
    return {'x': x, 'gamma': gamma, 'beta': beta, 'wq': wq, 'wkv': wkv, 'wo': wo, 'w1': w1, 'w3': w3, 'w2': w2}


def reference(x, gamma, beta, wq, wkv, wo, w1, w3, w2):
    qi = lax.broadcasted_iota(jnp.int32, (SEQ, SEQ), 0)
    ki = lax.broadcasted_iota(jnp.int32, (SEQ, SEQ), 1)
    causal = ki <= qi

    def one_seq(xs):
        xf = xs.astype(jnp.float32)
        mu = jnp.mean(xf, axis=-1, keepdims=True)
        var = jnp.mean(jnp.square(xf - mu), axis=-1, keepdims=True)
        ln = ((xf - mu) * lax.rsqrt(var + EPS) * gamma + beta).astype(jnp.bfloat16)
        q = jnp.dot(ln, wq, preferred_element_type=jnp.float32).astype(jnp.bfloat16)
        kv = jnp.dot(ln, wkv, preferred_element_type=jnp.float32).astype(jnp.bfloat16)
        k = kv[:, :HEAD]
        v = kv[:, HEAD:]

        def one_head(qh):
            s = jnp.dot(qh, k.T, preferred_element_type=jnp.float32) * HEAD ** -0.5
            s = jnp.where(causal, s, -1e30)
            p = jax.nn.softmax(s, axis=-1).astype(jnp.bfloat16)
            return jnp.dot(p, v, preferred_element_type=jnp.float32).astype(jnp.bfloat16)

        o = lax.map(one_head, q.reshape(SEQ, HEADS, HEAD).transpose(1, 0, 2))
        o = o.transpose(1, 0, 2).reshape(SEQ, HEADS * HEAD)
        a = jnp.dot(o, wo, preferred_element_type=jnp.float32)
        g = jnp.dot(ln, w1, preferred_element_type=jnp.float32)
        u = jnp.dot(ln, w3, preferred_element_type=jnp.float32)
        hm = (jax.nn.silu(g) * u).astype(jnp.bfloat16)
        m = jnp.dot(hm, w2, preferred_element_type=jnp.float32)
        return (xf + a + m).astype(jnp.bfloat16)

    return lax.map(one_seq, x)
```

```python
import functools

import jax
import jax.numpy as jnp
from jax import lax
from jax.experimental import pallas as pl
from jax.experimental.pallas import tpu as pltpu
from jax.sharding import PartitionSpec as P

EPS = 1e-5
MESH = pl.DeviceIdType.MESH
TOK = 256
LOG2E = 1.4426950408889634
F32 = jnp.float32
BF16 = jnp.bfloat16


def kernel(n_tp, seq,
           x, gamma, beta, wq, wkv, wo, w1, w3, w2,
           y,
           wqkv, w13, w2o, xin, lnst, ln, kv, act, part, pbuf, r1, r2, ybuf, xres,
           wsem, xsem, xrsem, lns, lnr, lnfree, kvs, kvr, ds_, dr_, s1s, s1r, s2s, s2r,
           ys, yr, fs, fr, gs, gr):
    d = x.shape[1]
    n = x.shape[0] // TOK
    per_seq = seq // TOK
    dq = wq.shape[1]
    dh = wkv.shape[1] // 2
    ff = w1.shape[1]
    nh = dq // dh
    half = TOK // 2
    chips = n_tp // 2
    blk = half // chips
    dm = d // 2

    me = lax.axis_index("tp")
    h = lax.rem(me, 2)
    c = me // 2
    cp = lax.rem(c + 1, chips)
    cm = lax.rem(c + chips - 1, chips)
    co = lax.rem(c + 2, chips)
    plus, minus, partner = cp * 2 + h, cm * 2 + h, c * 2 + 1 - h

    def rcopy(src, dst, ssem, rsem, dev):
        return pltpu.make_async_remote_copy(src_ref=src, dst_ref=dst, send_sem=ssem, recv_sem=rsem,
                                            device_id={"tp": dev}, device_id_type=MESH)

    def own(ref):
        return ref.at[pl.ds(pl.multiple_of(h * half, half), half)]

    def other(ref):
        return ref.at[pl.ds(pl.multiple_of((1 - h) * half, half), half)]

    def rows_of(k):
        return pl.ds(pl.multiple_of(k * blk, blk), blk)

    def yrows(j, k):
        return pl.ds(pl.multiple_of(j * TOK + h * half + k * blk, blk), blk)

    def x_copy(j):
        return pltpu.make_async_copy(x.at[pl.ds(pl.multiple_of(j * TOK + h * half, half), half)], xin, xsem)

    def xres_copy(j):
        return pltpu.make_async_copy(x.at[yrows(j, c)], xres.at[lax.rem(j, 2)], xrsem.at[lax.rem(j, 2)])

    w_copies = (
        pltpu.make_async_copy(wq, wqkv.at[:, pl.ds(0, dq)], wsem.at[0]),
        pltpu.make_async_copy(wkv.at[:, pl.ds(pl.multiple_of(h * dh, dh), dh)], wqkv.at[:, pl.ds(dq, dh)], wsem.at[1]),
        pltpu.make_async_copy(w1, w13.at[:, pl.ds(0, ff)], wsem.at[2]),
        pltpu.make_async_copy(w3, w13.at[:, pl.ds(ff, ff)], wsem.at[3]),
        pltpu.make_async_copy(wo, w2o.at[pl.ds(0, dq)], wsem.at[4]),
        pltpu.make_async_copy(w2, w2o.at[pl.ds(dq, ff)], wsem.at[5]),
    )

    def layer_norm():
        for r in range(0, half, 16):
            xf = xin[r:r + 16, :].astype(F32)
            mu = jnp.mean(xf, axis=-1, keepdims=True)
            xc = xf - mu
            var = jnp.mean(jnp.square(xc), axis=-1, keepdims=True)
            lnst[r:r + 16, :] = (xc * lax.rsqrt(var + EPS) * gamma[...] + beta[...]).astype(BF16)

    def ln_local():
        ln[pl.ds(pl.multiple_of(h * half, half), half), :] = lnst[...]

    def ln_copy():
        return rcopy(lnst, own(ln), lns, lnr, partner)

    def kv_copy(t):
        view = kv.at[h, pl.ds(pl.multiple_of(lax.rem(t, per_seq) * TOK, TOK), TOK)]
        return rcopy(view, view, kvs, kvr, partner)

    def d2d_copy(j):
        s = lax.rem(j, 2)
        return rcopy(other(part), pbuf.at[s], ds_.at[s], dr_.at[s], partner)

    def s1_copies(j):
        s = lax.rem(j, 2)
        return (rcopy(pbuf.at[s, rows_of(co), pl.ds(0, dm)], r1.at[s, 0], s1s.at[s, 0], s1r.at[s, 0], plus),
                rcopy(pbuf.at[s, rows_of(co), pl.ds(dm, dm)], r1.at[s, 1], s1s.at[s, 1], s1r.at[s, 1], minus))

    def s2_copies(j):
        s = lax.rem(j, 2)
        return (rcopy(pbuf.at[s, rows_of(cp)], r2.at[s, 0], s2s.at[s, 0], s2r.at[s, 0], plus),
                rcopy(pbuf.at[s, rows_of(cm)], r2.at[s, 1], s2s.at[s, 1], s2r.at[s, 1], minus))

    def y_copies(j, ks):
        s, s3 = lax.rem(j, 2), lax.rem(j, 3)
        return tuple(rcopy(ybuf.at[s], y.at[yrows(j, k)], ys.at[s3, i], yr.at[s3, i], dev)
                     for i, (k, dev) in enumerate(zip(ks, (plus, minus, partner))))

    def y_local(j):
        return pltpu.make_async_copy(ybuf.at[lax.rem(j, 2)], y.at[yrows(j, c)], ys.at[lax.rem(j, 3), 3])

    def f_copies(j):
        s3 = lax.rem(j, 3)
        va = y.at[yrows(j, cm), pl.ds(0, dm)]
        vb = y.at[yrows(j, cp), pl.ds(dm, dm)]
        vm, vp = y.at[yrows(j, cm)], y.at[yrows(j, cp)]
        return (rcopy(va, va, fs.at[s3, 0], fr.at[s3, 0], plus),
                rcopy(vb, vb, fs.at[s3, 1], fr.at[s3, 1], minus),
                rcopy(vm, vm, fs.at[s3, 2], fr.at[s3, 2], partner),
                rcopy(vp, vp, fs.at[s3, 3], fr.at[s3, 3], partner))

    def g_copy(j):
        s3 = lax.rem(j, 3)
        v = y.at[yrows(j, co)]
        return rcopy(v, v, gs.at[s3], gr.at[s3], partner)

    def s1(j):
        s = lax.rem(j, 2)
        cpy = d2d_copy(j)
        cpy.wait_recv()
        cpy.wait_send()

        @pl.loop(0, half // 32)
        def _(i):
            a = part[pl.ds(pl.multiple_of(h * half + i * 32, 32), 32), :].astype(F32)
            rr = pl.ds(pl.multiple_of(i * 32, 32), 32)
            pbuf[s, rr, :] = (a + pbuf[s, rr, :].astype(F32)).astype(BF16)

        for cpy in s1_copies(j):
            cpy.start()
        xres_copy(j).start()

    def s2(j):
        s = lax.rem(j, 2)
        first = s1_copies(j)
        for cpy in first:
            cpy.wait_recv()
        pbuf[s, rows_of(cp), :dm] = (pbuf[s, rows_of(cp), :dm].astype(F32) + r1[s, 0].astype(F32)).astype(BF16)
        pbuf[s, rows_of(cm), dm:] = (pbuf[s, rows_of(cm), dm:].astype(F32) + r1[s, 1].astype(F32)).astype(BF16)
        for cpy in s2_copies(j):
            cpy.start()
        for cpy in first:
            cpy.wait_send()

    def s3(j):
        s = lax.rem(j, 2)
        second = s2_copies(j)
        for cpy in second:
            cpy.wait_recv()
        xres_copy(j).wait()
        ybuf[s] = (xres[s].astype(F32) + ((pbuf[s, rows_of(c), :].astype(F32) + r2[s, 0].astype(F32))
                                          + r2[s, 1].astype(F32))).astype(BF16)
        for cpy in y_copies(j, (c, c, c)):
            cpy.start()
        y_local(j).start()
        for cpy in second:
            cpy.wait_send()

    def s4(j):
        for cpy in y_copies(j, (cm, cp, c)):
            cpy.wait_recv()
        for cpy in f_copies(j):
            cpy.start()
        for cpy in y_copies(j, (c, c, c)):
            cpy.wait_send()
        y_local(j).wait()

    def s5(j):
        for cpy in f_copies(j):
            cpy.wait_recv()
        g_copy(j).start()
        for cpy in f_copies(j):
            cpy.wait_send()

    def s6(j):
        g_copy(j).wait_recv()
        g_copy(j).wait_send()

    def attention(blocks):
        keys = blocks * TOK
        k = kv[0, :keys, :]
        v = kv[1, :keys, :]
        qi = lax.broadcasted_iota(jnp.int32, (TOK, TOK), 0)
        ki = lax.broadcasted_iota(jnp.int32, (TOK, TOK), 1)
        for a in range(nh):
            q = act[:, a * dh:(a + 1) * dh]
            sc = lax.dot_general(q, k, (((1,), (1,)), ((), ())), preferred_element_type=F32)
            sc = sc * (dh ** -0.5 * LOG2E)
            last = jnp.where(ki <= qi, sc[:, keys - TOK:], -1e30)
            sc = last if blocks == 1 else jnp.concatenate([sc[:, :keys - TOK], last], axis=1)
            p = jnp.exp2(sc - jnp.max(sc, axis=-1, keepdims=True))
            p = (p * (1.0 / jnp.sum(p, axis=-1, keepdims=True))).astype(BF16)
            act[:, a * dh:(a + 1) * dh] = jnp.dot(p, v, preferred_element_type=F32).astype(BF16)

    barrier = pltpu.get_barrier_semaphore()
    for dev in (partner, plus, minus):
        pl.semaphore_signal(barrier, inc=1, device_id={"tp": dev}, device_id_type=MESH)
    x_copy(0).start()
    for cpy in w_copies:
        cpy.start()
    pl.semaphore_wait(barrier, 3)
    x_copy(0).wait()
    layer_norm()
    ln_local()
    x_copy(1).start()
    ln_copy().start()

    @pl.loop(0, n + 5)
    def _(t):
        @pl.when(t < n)
        def _():
            ln_copy().wait_recv()
            ln_copy().wait_send()

            @pl.when(t == 0)
            def _():
                w_copies[0].wait()
                w_copies[1].wait()

            @pl.when(t + 1 < n)
            def _():
                x_copy(t + 1).wait()

            layer_norm()
            pos = pl.multiple_of(lax.rem(t, per_seq) * TOK, TOK)
            qkv = jnp.dot(ln[...], wqkv[...], preferred_element_type=F32).astype(BF16)
            act[:, :dq] = qkv[:, :dq]
            kv[h, pl.ds(pos, TOK), :] = qkv[:, dq:]

            @pl.when(t + 2 < n)
            def _():
                x_copy(t + 2).start()

        @pl.when((t >= 1) & (t <= n))
        def _():
            s1(t - 1)

        @pl.when((t >= 2) & (t <= n + 1))
        def _():
            s3(t - 2)

        @pl.when(t < n)
        def _():
            kv_copy(t).start()

            @pl.when(t == 0)
            def _():
                w_copies[2].wait()
                w_copies[3].wait()

            lhs = ln[...]
            tile = min(256, ff)
            for j in range(0, ff, tile):
                g = jnp.dot(lhs, w13[:, j:j + tile], preferred_element_type=F32)
                u = jnp.dot(lhs, w13[:, ff + j:ff + j + tile], preferred_element_type=F32)
                act[:, dq + j:dq + j + tile] = (jax.nn.silu(g) * u).astype(BF16)

            @pl.when(t + 1 < n)
            def _():
                pl.semaphore_signal(lnfree, inc=1, device_id={"tp": partner}, device_id_type=MESH)
                ln_local()

        @pl.when((t >= 1) & (t <= n))
        def _():
            s2(t - 1)

        @pl.when((t >= 3) & (t <= n + 2))
        def _():
            s4(t - 3)

        @pl.when((t >= 4) & (t <= n + 3))
        def _():
            s5(t - 4)

        @pl.when(t >= 5)
        def _():
            s6(t - 5)

        @pl.when(t < n)
        def _():
            kv_copy(t).wait_recv()
            kv_copy(t).wait_send()
            for b in range(per_seq):
                pl.when(lax.rem(t, per_seq) == b)(functools.partial(attention, b + 1))

            @pl.when(t + 1 < n)
            def _():
                pl.semaphore_wait(lnfree, 1)
                ln_copy().start()

            @pl.when(t == 0)
            def _():
                w_copies[4].wait()
                w_copies[5].wait()

            lhs = act[...]
            tile = min(512, d)
            for j in range(0, d, tile):
                part[:, j:j + tile] = jnp.dot(lhs, w2o[:, j:j + tile], preferred_element_type=F32).astype(BF16)
            d2d_copy(t).start()


def solution(mesh):
    n_tp = mesh.shape["tp"]

    def local(x, gamma, beta, wq, wkv, wo, w1, w3, w2):
        b, s, d = x.shape
        dq, dh, ff = wq.shape[1], wkv.shape[1] // 2, w1.shape[1]
        half = TOK // 2
        blk = half // (n_tp // 2)
        dma = pltpu.SemaphoreType.DMA
        hbm = pl.BlockSpec(memory_space=pl.ANY)
        vmem = pl.BlockSpec(memory_space=pltpu.VMEM)
        out = pl.pallas_call(
            functools.partial(kernel, n_tp, s),
            out_shape=jax.ShapeDtypeStruct((b * s, d), BF16),
            in_specs=[hbm, vmem, vmem] + [hbm] * 6,
            out_specs=hbm,
            scratch_shapes=[
                pltpu.VMEM((d, dq + dh), BF16),
                pltpu.VMEM((d, 2 * ff), BF16),
                pltpu.VMEM((dq + ff, d), BF16),
                pltpu.VMEM((half, d), BF16),
                pltpu.VMEM((half, d), BF16),
                pltpu.VMEM((TOK, d), BF16),
                pltpu.VMEM((2, s, dh), BF16),
                pltpu.VMEM((TOK, dq + ff), BF16),
                pltpu.VMEM((TOK, d), BF16),
                pltpu.VMEM((2, half, d), BF16),
                pltpu.VMEM((2, 2, blk, d // 2), BF16),
                pltpu.VMEM((2, 2, blk, d), BF16),
                pltpu.VMEM((2, blk, d), BF16),
                pltpu.VMEM((2, blk, d), BF16),
                dma((6,)), dma, dma((2,)), dma, dma, pltpu.SemaphoreType.REGULAR, dma, dma,
                dma((2,)), dma((2,)), dma((2, 2)), dma((2, 2)), dma((2, 2)), dma((2, 2)),
                dma((3, 4)), dma((3, 3)), dma((3, 4)), dma((3, 4)), dma((3,)), dma((3,)),
            ],
            compiler_params=pltpu.CompilerParams(collective_id=0, has_side_effects=True,
                                                 vmem_limit_bytes=67043328),
        )(x.reshape(b * s, d), gamma.reshape(1, d), beta.reshape(1, d), wq, wkv, wo, w1, w3, w2)
        return out.reshape(b, s, d)

    return jax.shard_map(local, mesh=mesh,
                         in_specs=(P('dp', None, None), P(), P(), P(None, 'tp'), P(), P('tp', None),
                                   P(None, 'tp'), P(None, 'tp'), P('tp', None)),
                         out_specs=P('dp', None, None), check_vma=False)
```

```python
import functools

import jax
import jax.numpy as jnp
from jax import lax
from jax.experimental import pallas as pl
from jax.experimental.pallas import tpu as pltpu
from jax.sharding import PartitionSpec as P

EPS = 1e-5
MESH = pl.DeviceIdType.MESH
TOK = 256
LOG2E = 1.4426950408889634
F32 = jnp.float32
BF16 = jnp.bfloat16
VMEM_LIMIT = 22 * 1024 * 1024


def kernel(n_tp, seq,
           x, gamma, beta, wq, wkv, wo, w1, w3, w2,
           y, wbuf,
           gb, wqkv, xin, lnst, ln, kv, act, part, pbuf, r1, r2, ybuf, xres,
           wsem, xsem, xrsem, lns, lnr, free, kvs, kvr, ds_, dr_, s1s, s1r, s2s, s2r, ts, tr,
           ys, yr, fs, fr, gs, gr, vsem):
    d = x.shape[1]
    n = x.shape[0] // TOK
    per_seq = seq // TOK
    dq = wq.shape[1]
    dh = wkv.shape[1] // 2
    ff = w1.shape[1]
    nh = dq // dh
    half = TOK // 2
    chips = n_tp // 2
    blk = half // chips
    dm = d // 2
    w13, w2o = wbuf.at[pl.ds(0, d)], wbuf.at[pl.ds(d, dq + ff)]

    me = lax.axis_index("tp")
    h = lax.rem(me, 2)
    c = me // 2
    cp = lax.rem(c + 1, chips)
    cm = lax.rem(c + chips - 1, chips)
    co = lax.rem(c + 2, chips)
    plus, minus, partner = cp * 2 + h, cm * 2 + h, c * 2 + 1 - h
    ca, cb = pl.ds(0, dm), pl.ds(dm, dm)

    def rcopy(src, dst, ssem, rsem, dev):
        return pltpu.make_async_remote_copy(src_ref=src, dst_ref=dst, send_sem=ssem, recv_sem=rsem,
                                            device_id={"tp": dev}, device_id_type=MESH)

    def own(ref):
        return ref.at[pl.ds(pl.multiple_of(h * half, half), half)]

    def rows_of(k):
        return pl.ds(pl.multiple_of(k * blk, blk), blk)

    def yrows(j, k):
        return pl.ds(pl.multiple_of(j * TOK + h * half + k * blk, blk), blk)

    def x_copy(j):
        return pltpu.make_async_copy(x.at[pl.ds(pl.multiple_of(j * TOK + h * half, half), half)], xin, xsem)

    def xres_copy(j):
        return pltpu.make_async_copy(x.at[yrows(j, c)], xres.at[lax.rem(j, 2)], xrsem.at[lax.rem(j, 2)])

    w_copies = (
        pltpu.make_async_copy(wq, wqkv.at[:, pl.ds(0, dq)], wsem.at[0]),
        pltpu.make_async_copy(wkv.at[:, pl.ds(pl.multiple_of(h * dh, dh), dh)], wqkv.at[:, pl.ds(dq, dh)], wsem.at[1]),
        pltpu.make_async_copy(w1, w13.at[:, pl.ds(0, ff)], wsem.at[2]),
        pltpu.make_async_copy(w3, w13.at[:, pl.ds(ff, ff)], wsem.at[3]),
        pltpu.make_async_copy(wo, w2o.at[pl.ds(0, dq)], wsem.at[4]),
        pltpu.make_async_copy(w2, w2o.at[pl.ds(dq, ff)], wsem.at[5]),
    )

    def layer_norm():
        for r in range(0, half, 16):
            xf = xin[r:r + 16, :].astype(F32)
            mu = jnp.mean(xf, axis=-1, keepdims=True)
            xc = xf - mu
            var = jnp.mean(jnp.square(xc), axis=-1, keepdims=True)
            lnst[r:r + 16, :] = (xc * lax.rsqrt(var + EPS) * gb[0:1, :] + gb[1:2, :]).astype(BF16)

    def ln_local():
        ln[pl.ds(pl.multiple_of(h * half, half), half), :] = lnst[...]

    def ln_copy():
        return rcopy(lnst, own(ln), lns, lnr, partner)

    def kv_copy(t):
        view = kv.at[h, pl.ds(pl.multiple_of(lax.rem(t, per_seq) * TOK, TOK), TOK)]
        return rcopy(view, view, kvs, kvr, partner)

    def d2d_copy(j, q):
        s = lax.rem(j, 2)
        cols = (ca, cb)[q]
        return rcopy(part.at[pl.ds(pl.multiple_of((1 - h) * half, half), half), cols], pbuf.at[s, :, cols],
                     ds_.at[s, q], dr_.at[s, q], partner)

    def s1_copies(j):
        s = lax.rem(j, 2)
        return (rcopy(pbuf.at[s, rows_of(co), ca], r1.at[s, 0], s1s.at[s, 0], s1r.at[s, 0], plus),
                rcopy(pbuf.at[s, rows_of(co), cb], r1.at[s, 1], s1s.at[s, 1], s1r.at[s, 1], minus))

    def t_copies(j):
        s = lax.rem(j, 2)
        return (rcopy(pbuf.at[s, rows_of(cp), cb], r2.at[s, 0, :, cb], ts.at[s, 0], tr.at[s, 0], plus),
                rcopy(pbuf.at[s, rows_of(cm), ca], r2.at[s, 1, :, ca], ts.at[s, 1], tr.at[s, 1], minus))

    def s2_copies(j):
        s = lax.rem(j, 2)
        return (rcopy(pbuf.at[s, rows_of(cp), ca], r2.at[s, 0, :, ca], s2s.at[s, 0], s2r.at[s, 0], plus),
                rcopy(pbuf.at[s, rows_of(cm), cb], r2.at[s, 1, :, cb], s2s.at[s, 1], s2r.at[s, 1], minus))

    def y_copies(j, k0, k1, k2):
        s = lax.rem(j, 2)
        parts = ((k0, ca, plus), (k1, cb, minus), (k0, cb, plus), (k1, ca, minus))
        out = [rcopy(ybuf.at[s, :, cols], y.at[yrows(j, k), cols], ys.at[s, i], yr.at[s, i], dev)
               for i, (k, cols, dev) in enumerate(parts)]
        return out + [rcopy(ybuf.at[s], y.at[yrows(j, k2)], ys.at[s, 4], yr.at[s, 4], partner)]

    def y_local(j):
        s = lax.rem(j, 2)
        return pltpu.make_async_copy(ybuf.at[s], y.at[yrows(j, c)], ys.at[s, 5])

    def f_copies(j):
        s = lax.rem(j, 2)
        va, vb = y.at[yrows(j, cm), ca], y.at[yrows(j, cp), cb]
        vm, vp = y.at[yrows(j, cm)], y.at[yrows(j, cp)]
        return (rcopy(va, va, fs.at[s, 0], fr.at[s, 0], plus),
                rcopy(vb, vb, fs.at[s, 1], fr.at[s, 1], minus),
                rcopy(vm, vm, fs.at[s, 2], fr.at[s, 2], partner),
                rcopy(vp, vp, fs.at[s, 3], fr.at[s, 3], partner))

    def g_copy(j):
        s3 = lax.rem(j, 3)
        v = y.at[yrows(j, co)]
        return rcopy(v, v, gs.at[s3], gr.at[s3], partner)

    def s1(j):
        s = lax.rem(j, 2)
        d2d_copy(j, 1).wait_recv()
        d2d_copy(j, 0).wait_send()
        d2d_copy(j, 1).wait_send()

        @pl.loop(0, half // 32)
        def _(i):
            a = part[pl.ds(pl.multiple_of(h * half + i * 32, 32), 32), :].astype(F32)
            rr = pl.ds(pl.multiple_of(i * 32, 32), 32)
            pbuf[s, rr, :] = (a + pbuf[s, rr, :].astype(F32)).astype(BF16)

        for cpy in s1_copies(j) + t_copies(j):
            cpy.start()
        xres_copy(j).start()

    def s2(j):
        s = lax.rem(j, 2)
        first = s1_copies(j)
        for cpy in first:
            cpy.wait_recv()
        pbuf[s, rows_of(cp), :dm] = (pbuf[s, rows_of(cp), :dm].astype(F32) + r1[s, 0].astype(F32)).astype(BF16)
        pbuf[s, rows_of(cm), dm:] = (pbuf[s, rows_of(cm), dm:].astype(F32) + r1[s, 1].astype(F32)).astype(BF16)
        for cpy in s2_copies(j):
            cpy.start()
        for cpy in first:
            cpy.wait_send()

    def s3(j):
        s = lax.rem(j, 2)
        copies = t_copies(j) + s2_copies(j)
        for cpy in copies:
            cpy.wait_recv()
        xres_copy(j).wait()
        ybuf[s] = (xres[s].astype(F32) + ((pbuf[s, rows_of(c), :].astype(F32) + r2[s, 0].astype(F32))
                                          + r2[s, 1].astype(F32))).astype(BF16)
        for cpy in y_copies(j, c, c, c):
            cpy.start()
        y_local(j).start()
        for cpy in copies:
            cpy.wait_send()

    def s4(j):
        came = y_copies(j, cm, cp, c)
        came[0].wait_recv()
        came[1].wait_recv()
        onward = f_copies(j)
        onward[0].start()
        onward[1].start()
        for cpy in came[2:]:
            cpy.wait_recv()
        onward[2].start()
        onward[3].start()
        for cpy in y_copies(j, c, c, c):
            cpy.wait_send()
        y_local(j).wait()

    def s5(j):
        for cpy in f_copies(j):
            cpy.wait_recv()
        g_copy(j).start()
        for cpy in f_copies(j):
            cpy.wait_send()

    def s6(j):
        g_copy(j).wait_recv()
        g_copy(j).wait_send()

    def hidden(j0, j1):
        lhs = ln[...]
        tile = min(256, ff)
        for j in range(j0 * tile, j1 * tile, tile):
            g = jnp.dot(lhs, w13[:, j:j + tile], preferred_element_type=F32)
            u = jnp.dot(lhs, w13[:, ff + j:ff + j + tile], preferred_element_type=F32)
            act[:, dq + j:dq + j + tile] = (jax.nn.silu(g) * u).astype(BF16)

    tiles = ff // min(256, ff)
    first_tiles = min(3, tiles - 1)

    def attend(t, blocks):
        keys = blocks * TOK
        k = kv[0, :keys, :]
        v = kv[1, :keys, :]
        open_ = max(keys - 2 * TOK, 0)
        qi = lax.broadcasted_iota(jnp.int32, (TOK, keys - open_), 0)
        ki = lax.broadcasted_iota(jnp.int32, (TOK, keys - open_), 1)
        seen = ki + open_ <= qi + lax.rem(t, per_seq) * TOK
        rest = list(range(first_tiles, tiles))
        for a in range(nh):
            q = act[:, a * dh:(a + 1) * dh]
            sc = lax.dot_general(q, k, (((1,), (1,)), ((), ())), preferred_element_type=F32)
            sc = sc * (dh ** -0.5 * LOG2E)
            if rest:
                j = rest.pop(0)
                hidden(j, j + 1)
            last = jnp.where(seen, sc[:, open_:], -1e30)
            sc = last if open_ == 0 else jnp.concatenate([sc[:, :open_], last], axis=1)
            p = jnp.exp2(sc - jnp.max(sc, axis=-1, keepdims=True))
            p = (p * (1.0 / jnp.sum(p, axis=-1, keepdims=True))).astype(BF16)
            if rest and a + 1 < nh:
                j = rest.pop(0)
                hidden(j, j + 1)
            act[:, a * dh:(a + 1) * dh] = jnp.dot(p, v, preferred_element_type=F32).astype(BF16)
        for j in rest:
            hidden(j, j + 1)

    in13, in_vmem = vmem_steps(n, d, dq, ff)
    early = max(min(in_vmem, n - 4), in13)

    def v_copy(j, steps, i):
        rows = pl.ds(j * TOK, steps * TOK)
        return pltpu.make_async_copy(y.at[rows], wbuf.at[rows], vsem.at[i])

    barrier = pltpu.get_barrier_semaphore()
    for dev in (partner, plus, minus):
        pl.semaphore_signal(barrier, inc=1, device_id={"tp": dev}, device_id_type=MESH)
    x_copy(0).start()
    for cpy in w_copies:
        cpy.start()
    gb[0:1, :] = gamma[...][None, :]
    gb[1:2, :] = beta[...][None, :]
    pl.semaphore_wait(barrier, 3)
    x_copy(0).wait()
    layer_norm()
    ln_local()
    x_copy(1).start()
    ln_copy().start()

    @pl.loop(0, n + 4)
    def _(t):
        @pl.when((t >= 1) & (t <= n))
        def _():
            d2d_copy(t - 1, 0).wait_recv()

        @pl.when(t < n)
        def _():
            ln_copy().wait_recv()
            ln_copy().wait_send()

            @pl.when(t == 0)
            def _():
                for cpy in w_copies[:4]:
                    cpy.wait()

            @pl.when(t + 1 < n)
            def _():
                x_copy(t + 1).wait()

            layer_norm()
            pos = lax.rem(t, per_seq)
            here = pl.ds(pl.multiple_of(pos * TOK, TOK), TOK)
            after = jnp.where(lax.rem(pos, 2) == 0, pos + 1, per_seq)
            kv[1, pl.ds(pl.multiple_of(after * TOK, TOK), TOK), :] = jnp.zeros((TOK, dh), BF16)
            qkv = jnp.dot(ln[...], wqkv[...], preferred_element_type=F32).astype(BF16)
            act[:, :dq] = qkv[:, :dq]
            kv[h, here, :] = qkv[:, dq:]
            kv_copy(t).start()
            hidden(0, first_tiles)

            @pl.when(t + 2 < n)
            def _():
                x_copy(t + 2).start()

        @pl.when((t >= 1) & (t <= n))
        def _():
            s1(t - 1)

        @pl.when(t < n)
        def _():
            kv_copy(t).wait_recv()
            kv_copy(t).wait_send()
            for b in range(0, per_seq, 2):
                pos = lax.rem(t, per_seq)
                pl.when((pos == b) | (pos == b + 1))(functools.partial(attend, t, b + 2))
            pl.semaphore_signal(free, inc=1, device_id={"tp": partner}, device_id_type=MESH)

            @pl.when(t + 1 < n)
            def _():
                ln_local()

            @pl.when(t == n - 1)
            def _():
                v_copy(0, in13, 0).start()

        @pl.when((t >= 1) & (t <= n))
        def _():
            s2(t - 1)

        @pl.when((t >= 2) & (t <= n + 1))
        def _():
            s4(t - 2)

        @pl.when(t < n)
        def _():
            pl.semaphore_wait(free, 1)

            @pl.when(t + 1 < n)
            def _():
                ln_copy().start()

            @pl.when(t == 0)
            def _():
                for cpy in w_copies[4:]:
                    cpy.wait()

            lhs = act[...]
            tile = min(256, dm)
            for q in range(2):
                for j in range(q * dm, (q + 1) * dm, tile):
                    part[:, j:j + tile] = jnp.dot(lhs, w2o[:, j:j + tile], preferred_element_type=F32).astype(BF16)
                d2d_copy(t, q).start()

        @pl.when((t >= 3) & (t <= n + 2))
        def _():
            s5(t - 3)

        @pl.when((t >= 1) & (t <= n))
        def _():
            s3(t - 1)

        @pl.when(t >= 4)
        def _():
            s6(t - 4)

        if early > in13:
            @pl.when(t == n - 1)
            def _():
                v_copy(in13, early - in13, 1).start()

        for i, j in enumerate(range(early, in_vmem)):
            @pl.when(t == j + 4)
            def _():
                v_copy(j, 1, 2 + i).start()

    v_copy(0, in13, 0).wait()
    if early > in13:
        v_copy(in13, early - in13, 1).wait()
    for i, j in enumerate(range(early, in_vmem)):
        v_copy(j, 1, 2 + i).wait()


def vmem_steps(n, d, dq, ff):
    in13 = d // TOK
    return in13, min(in13 + (dq + ff) // TOK, n - 1)


def finish(n, in_vmem, y, wbuf, out, buf, sem):
    loads = [pltpu.make_async_copy(y.at[pl.ds(j * TOK, TOK)], buf.at[j - in_vmem], sem.at[j]) for j in range(in_vmem, n)]
    stores = [pltpu.make_async_copy(wbuf.at[pl.ds(j * TOK, TOK)] if j < in_vmem else buf.at[j - in_vmem],
                                    out.at[pl.ds(j * TOK, TOK)], sem.at[n + j]) for j in range(n)]
    for cpy in loads + stores[:in_vmem]:
        cpy.start()
    for load, store in zip(loads, stores[in_vmem:]):
        load.wait()
        store.start()
    for cpy in stores:
        cpy.wait()


def solution(mesh):
    n_tp = mesh.shape["tp"]

    def local(x, gamma, beta, wq, wkv, wo, w1, w3, w2):
        b, s, d = x.shape
        dq, dh, ff = wq.shape[1], wkv.shape[1] // 2, w1.shape[1]
        n = b * s // TOK
        half = TOK // 2
        blk = half // (n_tp // 2)
        in13, in_vmem = vmem_steps(n, d, dq, ff)
        assert 2 * ff == d and in13 <= n - 5 and n_tp == 8
        dma = pltpu.SemaphoreType.DMA
        hbm = pl.BlockSpec(memory_space=pl.ANY)
        vmem = pl.BlockSpec(memory_space=pltpu.VMEM)
        y, wbuf = pl.pallas_call(
            functools.partial(kernel, n_tp, s),
            out_shape=(jax.ShapeDtypeStruct((b * s, d), BF16), pltpu.VMEM((d + dq + ff, d), BF16)),
            in_specs=[hbm, vmem, vmem] + [hbm] * 6,
            out_specs=(hbm, vmem),
            scratch_shapes=[
                pltpu.VMEM((2, d), F32),
                pltpu.VMEM((d, dq + dh), BF16),
                pltpu.VMEM((half, d), BF16),
                pltpu.VMEM((half, d), BF16),
                pltpu.VMEM((TOK, d), BF16),
                pltpu.VMEM((2, s + TOK, dh), BF16),
                pltpu.VMEM((TOK, dq + ff), BF16),
                pltpu.VMEM((TOK, d), BF16),
                pltpu.VMEM((2, half, d), BF16),
                pltpu.VMEM((2, 2, blk, d // 2), BF16),
                pltpu.VMEM((2, 2, blk, d), BF16),
                pltpu.VMEM((2, blk, d), BF16),
                pltpu.VMEM((2, blk, d), BF16),
                dma((6,)), dma, dma((2,)), dma, dma, pltpu.SemaphoreType.REGULAR, dma, dma,
                dma((2, 2)), dma((2, 2)), dma((2, 2)), dma((2, 2)), dma((2, 2)), dma((2, 2)), dma((2, 2)), dma((2, 2)),
                dma((2, 6)), dma((2, 5)), dma((2, 4)), dma((2, 4)), dma((3,)), dma((3,)), dma((6,)),
            ],
            compiler_params=pltpu.CompilerParams(collective_id=0, has_side_effects=True,
                                                 vmem_limit_bytes=VMEM_LIMIT),
        )(x.reshape(b * s, d), gamma, beta, wq, wkv, wo, w1, w3, w2)
        out = pl.pallas_call(
            functools.partial(finish, n, in_vmem),
            out_shape=jax.ShapeDtypeStruct((b * s, d), BF16),
            in_specs=[hbm, vmem],
            out_specs=hbm,
            scratch_shapes=[pltpu.VMEM((n - in_vmem, TOK, d), BF16), dma((2 * n,))],
            compiler_params=pltpu.CompilerParams(vmem_limit_bytes=8 * 1024 * 1024),
        )(y, wbuf)
        return out.reshape(b, s, d)

    return jax.shard_map(local, mesh=mesh,
                         in_specs=(P('dp', None, None), P(), P(), P(None, 'tp'), P(), P('tp', None),
                                   P(None, 'tp'), P(None, 'tp'), P('tp', None)),
                         out_specs=P('dp', None, None), check_vma=False)
```

```python
import functools

import jax
import jax.numpy as jnp
from jax import lax
from jax.experimental import pallas as pl
from jax.experimental.pallas import tpu as pltpu
from jax.sharding import PartitionSpec as P

EPS = 1e-5
MESH = pl.DeviceIdType.MESH
TOK = 256
LOG2E = 1.4426950408889634
F32 = jnp.float32
BF16 = jnp.bfloat16
VMEM_LIMIT = 24_800_000
BLOCK3 = 512


def kernel(n_tp, seq,
           x, gamma, beta, wq, wkv, wo, w1, w3, w2,
           y, wbuf,
           gb, wqkv, xin, lnst, ln, kv, act, part, pbuf, r1, r2, ybuf, xres,
           wsem, xsem, xrsem, lns, lnr, free, kvs, kvr, ds_, dr_, s1s, s1r, s2s, s2r, ts, tr,
           ys, yr, fs, fr, gs, gr, vsem):
    d = x.shape[1]
    n = x.shape[0] // TOK
    per_seq = seq // TOK
    dq = wq.shape[1]
    dh = wkv.shape[1] // 2
    ff = w1.shape[1]
    nh = dq // dh
    half = TOK // 2
    chips = n_tp // 2
    blk = half // chips
    dm = d // 2
    w13, w2o = wbuf.at[pl.ds(0, d)], wbuf.at[pl.ds(d, dq + ff)]

    me = lax.axis_index("tp")
    h = lax.rem(me, 2)
    c = me // 2
    cp = lax.rem(c + 1, chips)
    cm = lax.rem(c + chips - 1, chips)
    co = lax.rem(c + 2, chips)
    plus, minus, partner = cp * 2 + h, cm * 2 + h, c * 2 + 1 - h
    ca, cb = pl.ds(0, dm), pl.ds(dm, dm)
    cut = min(-(-d // 1024) * 512, d - 256)
    swap = ((0, cut), (cut, d))

    def rcopy(src, dst, ssem, rsem, dev):
        return pltpu.make_async_remote_copy(src_ref=src, dst_ref=dst, send_sem=ssem, recv_sem=rsem,
                                            device_id={"tp": dev}, device_id_type=MESH)

    def own(ref):
        return ref.at[pl.ds(pl.multiple_of(h * half, half), half)]

    def rows_of(k):
        return pl.ds(pl.multiple_of(k * blk, blk), blk)

    def yrows(j, k):
        return pl.ds(pl.multiple_of(j * TOK + h * half + k * blk, blk), blk)

    def x_copy(j):
        return pltpu.make_async_copy(x.at[pl.ds(pl.multiple_of(j * TOK + h * half, half), half)], xin, xsem)

    def xres_copy(j):
        return pltpu.make_async_copy(x.at[yrows(j, c)], xres.at[lax.rem(j, 2)], xrsem.at[lax.rem(j, 2)])

    w_copies = (
        pltpu.make_async_copy(wq, wqkv.at[:, pl.ds(0, dq)], wsem.at[0]),
        pltpu.make_async_copy(wkv.at[:, pl.ds(pl.multiple_of(h * dh, dh), dh)], wqkv.at[:, pl.ds(dq, dh)], wsem.at[1]),
        pltpu.make_async_copy(w1, w13.at[:, pl.ds(0, ff)], wsem.at[2]),
        pltpu.make_async_copy(w3, w13.at[:, pl.ds(ff, ff)], wsem.at[3]),
        pltpu.make_async_copy(wo, w2o.at[pl.ds(0, dq)], wsem.at[4]),
        pltpu.make_async_copy(w2, w2o.at[pl.ds(dq, ff)], wsem.at[5]),
    )

    def layer_norm(r0, r1):
        for r in range(r0, r1, 16):
            xf = xin[r:r + 16, :].astype(F32)
            mu = jnp.mean(xf, axis=-1, keepdims=True)
            xc = xf - mu
            var = jnp.mean(jnp.square(xc), axis=-1, keepdims=True)
            lnst[r:r + 16, :] = (xc * lax.rsqrt(var + EPS) * gb[0:1, :] + gb[1:2, :]).astype(BF16)

    def ln_local():
        ln[pl.ds(pl.multiple_of(h * half, half), half), :] = lnst[...]

    def ln_copy():
        return rcopy(lnst, own(ln), lns, lnr, partner)

    def kv_copy(t):
        view = kv.at[h, pl.ds(pl.multiple_of(lax.rem(t, per_seq) * TOK, TOK), TOK)]
        return rcopy(view, view, kvs, kvr, partner)

    def d2d_copy(j, q):
        s = lax.rem(j, 3)
        cols = pl.ds(swap[q][0], swap[q][1] - swap[q][0])
        return rcopy(part.at[pl.ds(pl.multiple_of((1 - h) * half, half), half), cols], pbuf.at[s, :, cols],
                     ds_.at[s, q], dr_.at[s, q], partner)

    def s1_copies(j):
        s, p = lax.rem(j, 2), lax.rem(j, 3)
        return (rcopy(pbuf.at[p, rows_of(co), ca], r1.at[s, 0], s1s.at[s, 0], s1r.at[s, 0], plus),
                rcopy(pbuf.at[p, rows_of(co), cb], r1.at[s, 1], s1s.at[s, 1], s1r.at[s, 1], minus))

    def t_copies(j):
        s = lax.rem(j, 3)
        return (rcopy(pbuf.at[s, rows_of(cp), cb], r2.at[s, 0, :, cb], ts.at[s, 0], tr.at[s, 0], plus),
                rcopy(pbuf.at[s, rows_of(cm), ca], r2.at[s, 1, :, ca], ts.at[s, 1], tr.at[s, 1], minus))

    def s2_copies(j):
        s = lax.rem(j, 3)
        return (rcopy(pbuf.at[s, rows_of(cp), ca], r2.at[s, 0, :, ca], s2s.at[s, 0], s2r.at[s, 0], plus),
                rcopy(pbuf.at[s, rows_of(cm), cb], r2.at[s, 1, :, cb], s2s.at[s, 1], s2r.at[s, 1], minus))

    def y_copies(j, k0, k1, k2):
        s, s3 = lax.rem(j, 2), lax.rem(j, 3)
        parts = ((k0, ca, plus), (k1, cb, minus), (k0, cb, plus), (k1, ca, minus))
        out = [rcopy(ybuf.at[s, :, cols], y.at[yrows(j, k), cols], ys.at[s, i], yr.at[s3, i], dev)
               for i, (k, cols, dev) in enumerate(parts)]
        return out + [rcopy(ybuf.at[s], y.at[yrows(j, k2)], ys.at[s, 4], yr.at[s3, 4], partner)]

    def y_local(j):
        s = lax.rem(j, 2)
        return pltpu.make_async_copy(ybuf.at[s], y.at[yrows(j, c)], ys.at[s, 5])

    def f_copies(j):
        s = lax.rem(j, 3)
        va, vb = y.at[yrows(j, cm), ca], y.at[yrows(j, cp), cb]
        vm, vp = y.at[yrows(j, cm)], y.at[yrows(j, cp)]
        return (rcopy(va, va, fs.at[s, 0], fr.at[s, 0], plus),
                rcopy(vb, vb, fs.at[s, 1], fr.at[s, 1], minus),
                rcopy(vm, vm, fs.at[s, 2], fr.at[s, 2], partner),
                rcopy(vp, vp, fs.at[s, 3], fr.at[s, 3], partner))

    def g_copy(j):
        s3 = lax.rem(j, 3)
        v = y.at[yrows(j, co)]
        return rcopy(v, v, gs.at[s3], gr.at[s3], partner)

    def s1(j):
        s = lax.rem(j, 3)
        d2d_copy(j, 1).wait_recv()
        d2d_copy(j, 0).wait_send()
        d2d_copy(j, 1).wait_send()

        @pl.loop(0, half // 32)
        def _(i):
            a = part[pl.ds(pl.multiple_of(h * half + i * 32, 32), 32), :].astype(F32)
            rr = pl.ds(pl.multiple_of(i * 32, 32), 32)
            pbuf[s, rr, :] = (a + pbuf[s, rr, :].astype(F32)).astype(BF16)

        for cpy in s1_copies(j) + t_copies(j):
            cpy.start()
        xres_copy(j).start()

    def s2(j):
        s, p = lax.rem(j, 2), lax.rem(j, 3)
        first = s1_copies(j)
        for cpy in first:
            cpy.wait_recv()
        pbuf[p, rows_of(cp), :dm] = (pbuf[p, rows_of(cp), :dm].astype(F32) + r1[s, 0].astype(F32)).astype(BF16)
        pbuf[p, rows_of(cm), dm:] = (pbuf[p, rows_of(cm), dm:].astype(F32) + r1[s, 1].astype(F32)).astype(BF16)
        for cpy in s2_copies(j):
            cpy.start()
        for cpy in first:
            cpy.wait_send()

    def s3(j):
        s, p = lax.rem(j, 2), lax.rem(j, 3)
        copies = t_copies(j) + s2_copies(j)
        for cpy in copies:
            cpy.wait_recv()
        xres_copy(j).wait()
        ybuf[s] = (xres[s].astype(F32) + ((pbuf[p, rows_of(c), :].astype(F32) + r2[p, 0].astype(F32))
                                          + r2[p, 1].astype(F32))).astype(BF16)
        for cpy in y_copies(j, c, c, c):
            cpy.start()
        y_local(j).start()
        for cpy in copies:
            cpy.wait_send()

    def s4(j):
        came = y_copies(j, cm, cp, c)
        came[0].wait_recv()
        came[1].wait_recv()
        onward = f_copies(j)
        onward[0].start()
        onward[1].start()
        for cpy in came[2:]:
            cpy.wait_recv()
        onward[2].start()
        onward[3].start()
        for cpy in y_copies(j, c, c, c):
            cpy.wait_send()
        y_local(j).wait()

    def s5(j):
        for cpy in f_copies(j):
            cpy.wait_recv()
        g_copy(j).start()
        for cpy in f_copies(j):
            cpy.wait_send()

    def s6(j):
        g_copy(j).wait_recv()
        g_copy(j).wait_send()

    def hidden(j0, j1):
        lhs = ln[...]
        tile = min(256, ff)
        for j in range(j0 * tile, j1 * tile, tile):
            g = jnp.dot(lhs, w13[:, j:j + tile], preferred_element_type=F32)
            u = jnp.dot(lhs, w13[:, ff + j:ff + j + tile], preferred_element_type=F32)
            act[:, dq + j:dq + j + tile] = (jax.nn.silu(g) * u).astype(BF16)

    tiles = ff // min(256, ff)
    first_tiles = min(3, tiles - 1)

    def attend(t, blocks):
        keys = blocks * TOK
        k = kv[0, :keys, :]
        v = kv[1, :keys, :]
        open_ = max(keys - 2 * TOK, 0)
        qi = lax.broadcasted_iota(jnp.int32, (TOK, keys - open_), 0)
        ki = lax.broadcasted_iota(jnp.int32, (TOK, keys - open_), 1)
        seen = ki + open_ <= qi + lax.rem(t, per_seq) * TOK
        rest = list(range(first_tiles, tiles))
        for a in range(nh):
            q = act[:, a * dh:(a + 1) * dh]
            sc = lax.dot_general(q, k, (((1,), (1,)), ((), ())), preferred_element_type=F32)
            sc = sc * (dh ** -0.5 * LOG2E)
            if rest:
                j = rest.pop(0)
                hidden(j, j + 1)
            last = jnp.where(seen, sc[:, open_:], -1e30)
            sc = last if open_ == 0 else jnp.concatenate([sc[:, :open_], last], axis=1)
            p = jnp.exp2(sc - jnp.max(sc, axis=-1, keepdims=True))
            p = (p * (1.0 / jnp.sum(p, axis=-1, keepdims=True))).astype(BF16)
            if rest and a + 1 < nh:
                j = rest.pop(0)
                hidden(j, j + 1)
            act[:, a * dh:(a + 1) * dh] = jnp.dot(p, v, preferred_element_type=F32).astype(BF16)
        for j in rest:
            hidden(j, j + 1)

    in13, in_vmem = vmem_steps(n, d, dq, ff)
    early = max(min(in_vmem, n - 5), in13)

    def v_copy(j, steps, i):
        rows = pl.ds(j * TOK, steps * TOK)
        return pltpu.make_async_copy(y.at[rows], wbuf.at[rows], vsem.at[i])

    barrier = pltpu.get_barrier_semaphore()
    for dev in (partner, plus, minus):
        pl.semaphore_signal(barrier, inc=1, device_id={"tp": dev}, device_id_type=MESH)
    x_copy(0).start()
    for cpy in w_copies:
        cpy.start()
    gb[0:1, :] = gamma[...][None, :]
    gb[1:2, :] = beta[...][None, :]
    pl.semaphore_wait(barrier, 3)
    x_copy(0).wait()
    layer_norm(0, half)
    ln_local()
    x_copy(1).start()
    ln_copy().start()

    @pl.loop(0, n + 5)
    def _(t):
        @pl.when((t >= 1) & (t <= n))
        def _():
            d2d_copy(t - 1, 0).wait_recv()

        @pl.when(t < n)
        def _():
            ln_copy().wait_recv()
            ln_copy().wait_send()

            @pl.when(t == 0)
            def _():
                for cpy in w_copies[:4]:
                    cpy.wait()

            @pl.when(t + 1 < n)
            def _():
                x_copy(t + 1).wait()

            pos = lax.rem(t, per_seq)
            after = jnp.where(lax.rem(pos, 2) == 0, pos + 1, per_seq)
            kv[1, pl.ds(pl.multiple_of(after * TOK, TOK), TOK), :] = jnp.zeros((TOK, dh), BF16)
            act[:, :dq] = jnp.dot(ln[...], wqkv[:, :dq], preferred_element_type=F32).astype(BF16)
            for r in range(0, TOK, half):
                kv[h, pl.ds(pl.multiple_of(pos * TOK + r, half), half), :] = jnp.dot(
                    ln[r:r + half, :], wqkv[:, dq:], preferred_element_type=F32).astype(BF16)
            kv_copy(t).start()
            step = half // first_tiles // 16 * 16
            for i in range(first_tiles):
                layer_norm(i * step, half if i + 1 == first_tiles else (i + 1) * step)
                hidden(i, i + 1)

            @pl.when(t + 2 < n)
            def _():
                x_copy(t + 2).start()

        @pl.when((t >= 1) & (t <= n))
        def _():
            s1(t - 1)

        @pl.when(t < n)
        def _():
            kv_copy(t).wait_recv()
            kv_copy(t).wait_send()
            for b in range(0, per_seq, 2):
                pos = lax.rem(t, per_seq)
                pl.when((pos == b) | (pos == b + 1))(functools.partial(attend, t, b + 2))
            pl.semaphore_signal(free, inc=1, device_id={"tp": partner}, device_id_type=MESH)

            @pl.when(t + 1 < n)
            def _():
                ln_local()

            @pl.when(t == n - 1)
            def _():
                v_copy(0, in13, 0).start()

        @pl.when((t >= 2) & (t <= n + 1))
        def _():
            s3(t - 2)

        @pl.when(t < n)
        def _():
            pl.semaphore_wait(free, 1)

            @pl.when(t + 1 < n)
            def _():
                ln_copy().start()

            @pl.when(t == 0)
            def _():
                for cpy in w_copies[4:]:
                    cpy.wait()

            lhs = act[...]
            for q, (c0, c1) in enumerate(swap):
                for j in range(c0, c1, BLOCK3):
                    e = min(j + BLOCK3, c1)
                    part[:, j:e] = jnp.dot(lhs, w2o[:, j:e], preferred_element_type=F32).astype(BF16)
                d2d_copy(t, q).start()

        @pl.when((t >= 1) & (t <= n))
        def _():
            s2(t - 1)

        @pl.when((t >= 3) & (t <= n + 2))
        def _():
            s4(t - 3)

        @pl.when((t >= 4) & (t <= n + 3))
        def _():
            s5(t - 4)

        @pl.when(t >= 5)
        def _():
            s6(t - 5)

        if early > in13:
            @pl.when(t == n - 1)
            def _():
                v_copy(in13, early - in13, 1).start()

        for i, j in enumerate(range(early, in_vmem)):
            @pl.when(t == j + 5)
            def _():
                v_copy(j, 1, 2 + i).start()

    v_copy(0, in13, 0).wait()
    if early > in13:
        v_copy(in13, early - in13, 1).wait()
    for i, j in enumerate(range(early, in_vmem)):
        v_copy(j, 1, 2 + i).wait()


def vmem_steps(n, d, dq, ff):
    in13 = d // TOK
    return in13, min(in13 + (dq + ff) // TOK, n - 1)


def finish(n, in_vmem, y, wbuf, out, buf, sem):
    loads = [pltpu.make_async_copy(y.at[pl.ds(j * TOK, TOK)], buf.at[j - in_vmem], sem.at[j]) for j in range(in_vmem, n)]
    stores = [pltpu.make_async_copy(wbuf.at[pl.ds(j * TOK, TOK)] if j < in_vmem else buf.at[j - in_vmem],
                                    out.at[pl.ds(j * TOK, TOK)], sem.at[n + j]) for j in range(n)]
    for cpy in loads + stores[:in_vmem]:
        cpy.start()
    for load, store in zip(loads, stores[in_vmem:]):
        load.wait()
        store.start()
    for cpy in stores:
        cpy.wait()


def solution(mesh):
    n_tp = mesh.shape["tp"]

    def local(x, gamma, beta, wq, wkv, wo, w1, w3, w2):
        b, s, d = x.shape
        dq, dh, ff = wq.shape[1], wkv.shape[1] // 2, w1.shape[1]
        n = b * s // TOK
        half = TOK // 2
        blk = half // (n_tp // 2)
        in13, in_vmem = vmem_steps(n, d, dq, ff)
        assert 2 * ff == d and in13 <= n - 6 and n_tp == 8
        dma = pltpu.SemaphoreType.DMA
        hbm = pl.BlockSpec(memory_space=pl.ANY)
        vmem = pl.BlockSpec(memory_space=pltpu.VMEM)
        y, wbuf = pl.pallas_call(
            functools.partial(kernel, n_tp, s),
            out_shape=(jax.ShapeDtypeStruct((b * s, d), BF16), pltpu.VMEM((d + dq + ff, d), BF16)),
            in_specs=[hbm, vmem, vmem] + [hbm] * 6,
            out_specs=(hbm, vmem),
            scratch_shapes=[
                pltpu.VMEM((2, d), F32),
                pltpu.VMEM((d, dq + dh), BF16),
                pltpu.VMEM((half, d), BF16),
                pltpu.VMEM((half, d), BF16),
                pltpu.VMEM((TOK, d), BF16),
                pltpu.VMEM((2, s + TOK, dh), BF16),
                pltpu.VMEM((TOK, dq + ff), BF16),
                pltpu.VMEM((TOK, d), BF16),
                pltpu.VMEM((3, half, d), BF16),
                pltpu.VMEM((2, 2, blk, d // 2), BF16),
                pltpu.VMEM((3, 2, blk, d), BF16),
                pltpu.VMEM((2, blk, d), BF16),
                pltpu.VMEM((2, blk, d), BF16),
                dma((6,)), dma, dma((2,)), dma, dma, pltpu.SemaphoreType.REGULAR, dma, dma,
                dma((3, 2)), dma((3, 2)), dma((2, 2)), dma((2, 2)), dma((3, 2)), dma((3, 2)), dma((3, 2)), dma((3, 2)),
                dma((2, 6)), dma((3, 5)), dma((3, 4)), dma((3, 4)), dma((3,)), dma((3,)), dma((7,)),
            ],
            compiler_params=pltpu.CompilerParams(collective_id=0, has_side_effects=True, vmem_limit_bytes=VMEM_LIMIT),
        )(x.reshape(b * s, d), gamma, beta, wq, wkv, wo, w1, w3, w2)
        out = pl.pallas_call(
            functools.partial(finish, n, in_vmem),
            out_shape=jax.ShapeDtypeStruct((b * s, d), BF16),
            in_specs=[hbm, vmem],
            out_specs=hbm,
            scratch_shapes=[pltpu.VMEM((n - in_vmem, TOK, d), BF16), dma((2 * n,))],
            compiler_params=pltpu.CompilerParams(vmem_limit_bytes=8 * 1024 * 1024),
        )(y, wbuf)
        return out.reshape(b, s, d)

    return jax.shard_map(local, mesh=mesh,
                         in_specs=(P('dp', None, None), P(), P(), P(None, 'tp'), P(), P('tp', None),
                                   P(None, 'tp'), P(None, 'tp'), P('tp', None)),
                         out_specs=P('dp', None, None), check_vma=False)
```

```python
import functools

import jax
import jax.numpy as jnp
from jax import lax
from jax.experimental import pallas as pl
from jax.experimental.pallas import tpu as pltpu
from jax.sharding import PartitionSpec as P

EPS = 1e-5
MESH = pl.DeviceIdType.MESH
TOK = 256
LOG2E = 1.4426950408889634
F32 = jnp.float32
BF16 = jnp.bfloat16
VMEM_LIMIT = 24_800_000
BLOCK3 = 512


def kernel(n_tp, seq,
           x, gamma, beta, wq, wkv, wo, w1, w3, w2,
           y, wbuf,
           gb, wqkv, xin, lnst, ln, kv, act, part, pbuf, r1, r2, ybuf,
           wsem, xsem, xrsem, lns, lnr, free, kvs, kvr, ds_, dr_, us, ur, s1r,
           ys, yr, fs, fr, gs, gr, vsem):
    d = x.shape[1]
    n = x.shape[0] // TOK
    per_seq = seq // TOK
    dq = wq.shape[1]
    dh = wkv.shape[1] // 2
    ff = w1.shape[1]
    nh = dq // dh
    half = TOK // 2
    chips = n_tp // 2
    blk = half // chips
    dm = d // 2
    w13, w2o = wbuf.at[pl.ds(0, d)], wbuf.at[pl.ds(d, dq + ff)]

    me = lax.axis_index("tp")
    h = lax.rem(me, 2)
    c = me // 2
    cp = lax.rem(c + 1, chips)
    cm = lax.rem(c + chips - 1, chips)
    co = lax.rem(c + 2, chips)
    plus, minus, partner = cp * 2 + h, cm * 2 + h, c * 2 + 1 - h
    ca, cb = pl.ds(0, dm), pl.ds(dm, dm)

    def rcopy(src, dst, ssem, rsem, dev):
        return pltpu.make_async_remote_copy(src_ref=src, dst_ref=dst, send_sem=ssem, recv_sem=rsem,
                                            device_id={"tp": dev}, device_id_type=MESH)

    def own(ref):
        return ref.at[pl.ds(pl.multiple_of(h * half, half), half)]

    def rows_of(k):
        return pl.ds(pl.multiple_of(k * blk, blk), blk)

    def yrows(j, k):
        return pl.ds(pl.multiple_of(j * TOK + h * half + k * blk, blk), blk)

    def x_copy(j):
        return pltpu.make_async_copy(x.at[pl.ds(pl.multiple_of(j * TOK + h * half, half), half)], xin, xsem)

    def xres_copy(j):
        return pltpu.make_async_copy(x.at[yrows(j, c)], ybuf, xrsem)

    w_copies = (
        pltpu.make_async_copy(wq, wqkv.at[:, pl.ds(0, dq)], wsem.at[0]),
        pltpu.make_async_copy(wkv.at[:, pl.ds(pl.multiple_of(h * dh, dh), dh)], wqkv.at[:, pl.ds(dq, dh)], wsem.at[1]),
        pltpu.make_async_copy(w1, w13.at[:, pl.ds(0, ff)], wsem.at[2]),
        pltpu.make_async_copy(w3, w13.at[:, pl.ds(ff, ff)], wsem.at[3]),
        pltpu.make_async_copy(wo, w2o.at[pl.ds(0, dq)], wsem.at[4]),
        pltpu.make_async_copy(w2, w2o.at[pl.ds(dq, ff)], wsem.at[5]),
    )

    def layer_norm(r0, r1):
        for r in range(r0, r1, 16):
            xf = xin[r:r + 16, :].astype(F32)
            mu = jnp.mean(xf, axis=-1, keepdims=True)
            xc = xf - mu
            var = jnp.mean(jnp.square(xc), axis=-1, keepdims=True)
            lnst[r:r + 16, :] = (xc * lax.rsqrt(var + EPS) * gb[0:1, :] + gb[1:2, :]).astype(BF16)

    def ln_local():
        ln[pl.ds(pl.multiple_of(h * half, half), half), :] = lnst[...]

    def ln_copy():
        return rcopy(lnst, own(ln), lns, lnr, partner)

    def kv_copy(t):
        view = kv.at[h, pl.ds(pl.multiple_of(lax.rem(t, per_seq) * TOK, TOK), TOK)]
        return rcopy(view, view, kvs, kvr, partner)

    def got(sem, k):
        view = part.at[pl.ds(0, k * blk)]
        rcopy(view, view, sem, sem, partner).wait_recv()

    def sent(sem, k):
        view = part.at[pl.ds(0, k * blk)]
        rcopy(view, view, sem, sem, partner).wait_send()

    def d2d_copy(j):
        p = lax.rem(j, 3)
        return rcopy(part.at[pl.ds(pl.multiple_of((1 - h) * half, half), half)], pbuf.at[p], ds_.at[p], dr_.at[p], partner)

    def ways(j):
        even = lax.rem(j, 2) == 0
        pick = lambda u, v: jnp.where(even, u, v)
        return pick(plus, minus), pick(minus, plus), pick(cp, cm), pick(cm, cp), pick(0, 1), pick(1, 0)

    def s1_add(j):
        p = lax.rem(j, 3)
        got(dr_.at[p], chips)
        sent(ds_.at[p], chips)

        @pl.loop(0, half // 32)
        def _(i):
            mine = part[pl.ds(pl.multiple_of(h * half + i * 32, 32), 32), :]
            rr = pl.ds(pl.multiple_of(i * 32, 32), 32)
            pbuf[p, rr, :] = mine + pbuf[p, rr, :]

    def s1(j):
        p = lax.rem(j, 3)
        ahead, behind, _, k_behind, _, i_behind = ways(j)
        s1_add(j)
        rcopy(pbuf.at[p, rows_of(co)], r1.at[p], us.at[p], s1r.at[p], ahead).start()
        rcopy(pbuf.at[p, rows_of(k_behind)], r2.at[p, i_behind], us.at[p], ur.at[p], behind).start()

    def s2(j):
        p = lax.rem(j, 3)
        ahead, _, k_ahead, _, i_ahead, _ = ways(j)
        got(s1r.at[p], 1)
        pbuf[p, rows_of(k_ahead), :] = pbuf[p, rows_of(k_ahead), :] + r1[p]
        rcopy(pbuf.at[p, rows_of(k_ahead)], r2.at[p, i_ahead], us.at[p], ur.at[p], ahead).start()

    def residual(j):
        @pl.when(j >= 1)
        def _():
            sent(ys, 3)

        xres_copy(j).start()

    def s3_sum(j):
        p = lax.rem(j, 3)
        got(ur.at[p], 2)
        xres_copy(j).wait()
        ybuf[...] = (ybuf[...].astype(F32) + ((pbuf[p, rows_of(c), :].astype(F32) + r2[p, 0].astype(F32))
                                          + r2[p, 1].astype(F32))).astype(BF16)

    def y_local(j):
        pltpu.make_async_copy(ybuf, y.at[yrows(j, c)], ys).start()

    def s3(j):
        p = lax.rem(j, 3)
        s3_sum(j)
        for dev in (plus, minus):
            rcopy(ybuf, y.at[yrows(j, c)], ys, yr.at[p], dev).start()
        y_local(j)
        sent(us.at[p], 3)

    def s4(j):
        p = lax.rem(j, 3)
        _, behind, k_ahead, _, _, _ = ways(j)
        got(yr.at[p], 2)
        view = y.at[yrows(j, k_ahead)]
        rcopy(view, view, fs.at[p], fr.at[p], behind).start()

    def s5(j):
        p = lax.rem(j, 3)
        got(fr.at[p], 1)
        view = y.at[pl.ds(pl.multiple_of(j * TOK + h * half, half), half)]
        rcopy(view, view, gs.at[p], gr.at[p], partner).start()
        sent(fs.at[p], 1)

    def s6(j):
        p = lax.rem(j, 3)
        got(gr.at[p], chips)
        sent(gs.at[p], chips)

    def s1_last(j):
        p = lax.rem(j, 3)
        s1_add(j)
        rcopy(pbuf.at[p, rows_of(co), ca], r1.at[p, :, ca], us.at[p], s1r.at[p], plus).start()
        rcopy(pbuf.at[p, rows_of(co), cb], r1.at[p, :, cb], us.at[p], s1r.at[p], minus).start()
        rcopy(pbuf.at[p, rows_of(cp), cb], r2.at[p, 0, :, cb], us.at[p], ur.at[p], plus).start()
        rcopy(pbuf.at[p, rows_of(cm), ca], r2.at[p, 1, :, ca], us.at[p], ur.at[p], minus).start()

    def s2_last(j):
        p = lax.rem(j, 3)
        got(s1r.at[p], 1)
        pbuf[p, rows_of(cp), :dm] = pbuf[p, rows_of(cp), :dm] + r1[p, :, :dm]
        pbuf[p, rows_of(cm), dm:] = pbuf[p, rows_of(cm), dm:] + r1[p, :, dm:]
        rcopy(pbuf.at[p, rows_of(cp), ca], r2.at[p, 0, :, ca], us.at[p], ur.at[p], plus).start()
        rcopy(pbuf.at[p, rows_of(cm), cb], r2.at[p, 1, :, cb], us.at[p], ur.at[p], minus).start()

    def s3_last(j):
        p = lax.rem(j, 3)
        s3_sum(j)
        for cols, sem, dev in ((ca, yr.at[p], plus), (cb, yr.at[p], minus), (cb, yr.at[3], plus), (ca, yr.at[3], minus)):
            rcopy(ybuf.at[:, cols], y.at[yrows(j, c), cols], ys, sem, dev).start()
        y_local(j)
        sent(us.at[p], 3)

    def s4_last(j):
        p = lax.rem(j, 3)
        got(yr.at[p], 1)
        for k, cols, dev in ((cm, ca, plus), (cp, cb, minus)):
            view = y.at[yrows(j, k), cols]
            rcopy(view, view, fs.at[p], fr.at[p], dev).start()
        got(yr.at[3], 1)
        sent(ys, 3)

    def hidden(j0, j1):
        lhs = ln[...]
        tile = min(256, ff)
        for j in range(j0 * tile, j1 * tile, tile):
            g = jnp.dot(lhs, w13[:, j:j + tile], preferred_element_type=F32)
            u = jnp.dot(lhs, w13[:, ff + j:ff + j + tile], preferred_element_type=F32)
            act[:, dq + j:dq + j + tile] = (jax.nn.silu(g) * u).astype(BF16)

    tiles = ff // min(256, ff)
    first_tiles = min(3, tiles - 1)

    def attend(t, blocks):
        keys = blocks * TOK
        k = kv[0, :keys, :]
        v = kv[1, :keys, :]
        open_ = max(keys - 2 * TOK, 0)
        qi = lax.broadcasted_iota(jnp.int32, (TOK, keys - open_), 0)
        ki = lax.broadcasted_iota(jnp.int32, (TOK, keys - open_), 1)
        seen = ki + open_ <= qi + lax.rem(t, per_seq) * TOK
        rest = list(range(first_tiles, tiles))
        for a in range(nh):
            q = act[:, a * dh:(a + 1) * dh]
            sc = lax.dot_general(q, k, (((1,), (1,)), ((), ())), preferred_element_type=F32)
            sc = sc * (dh ** -0.5 * LOG2E)
            if rest:
                j = rest.pop(0)
                hidden(j, j + 1)
            last = jnp.where(seen, sc[:, open_:], -1e30)
            sc = last if open_ == 0 else jnp.concatenate([sc[:, :open_], last], axis=1)
            p = jnp.exp2(sc - jnp.max(sc, axis=-1, keepdims=True))
            p = (p * (1.0 / jnp.sum(p, axis=-1, keepdims=True))).astype(BF16)
            if rest and a + 1 < nh:
                j = rest.pop(0)
                hidden(j, j + 1)
            act[:, a * dh:(a + 1) * dh] = jnp.dot(p, v, preferred_element_type=F32).astype(BF16)
        for j in rest:
            hidden(j, j + 1)

    in13, in_vmem = vmem_steps(n, d, dq, ff)
    early = min(in_vmem, n - 5)

    def v_copy(j, steps, i):
        rows = pl.ds(j * TOK, steps * TOK)
        return pltpu.make_async_copy(y.at[rows], wbuf.at[rows], vsem.at[i])

    barrier = pltpu.get_barrier_semaphore()
    for dev in (partner, plus, minus):
        pl.semaphore_signal(barrier, inc=1, device_id={"tp": dev}, device_id_type=MESH)
    x_copy(0).start()
    for cpy in w_copies:
        cpy.start()
    gb[0:1, :] = gamma[...][None, :]
    gb[1:2, :] = beta[...][None, :]
    pl.semaphore_wait(barrier, 3)
    x_copy(0).wait()
    layer_norm(0, half)
    ln_local()
    x_copy(1).start()
    ln_copy().start()

    @pl.loop(0, n)
    def _(t):
        ln_copy().wait_recv()
        ln_copy().wait_send()

        @pl.when(t == 0)
        def _():
            for cpy in w_copies[:4]:
                cpy.wait()

        @pl.when(t + 1 < n)
        def _():
            x_copy(t + 1).wait()

        pos = lax.rem(t, per_seq)

        @pl.when(lax.rem(pos, 2) == 0)
        def _():
            kv[1, pl.ds(pl.multiple_of((pos + 1) * TOK, TOK), TOK), :] = jnp.zeros((TOK, dh), BF16)

        act[:, :dq] = jnp.dot(ln[...], wqkv[:, :dq], preferred_element_type=F32).astype(BF16)
        for r in range(0, TOK, half):
            kv[h, pl.ds(pl.multiple_of(pos * TOK + r, half), half), :] = jnp.dot(
                ln[r:r + half, :], wqkv[:, dq:], preferred_element_type=F32).astype(BF16)
        kv_copy(t).start()
        step = half // max(first_tiles, 1) // 16 * 16
        for i in range(first_tiles):
            layer_norm(i * step, (i + 1) * step)
            hidden(i, i + 1)
        layer_norm(first_tiles * step, half)

        @pl.when(t + 2 < n)
        def _():
            x_copy(t + 2).start()

        @pl.when(t >= 1)
        def _():
            s1(t - 1)

        @pl.when(t >= 2)
        def _():
            residual(t - 2)

        kv_copy(t).wait_recv()
        kv_copy(t).wait_send()
        for b in range(0, per_seq, 2):
            pl.when((pos == b) | (pos == b + 1))(functools.partial(attend, t, b + 2))
        pl.semaphore_signal(free, inc=1, device_id={"tp": partner}, device_id_type=MESH)

        @pl.when(t >= 2)
        def _():
            s3(t - 2)

        pl.semaphore_wait(free, 1)

        @pl.when(t == 0)
        def _():
            for cpy in w_copies[4:]:
                cpy.wait()

        @pl.when(t == n - 1)
        def _():
            v_copy(0, in13, 0).start()

        @pl.when(t + 1 < n)
        def _():
            ln_copy().start()

        ln_local()
        lhs = act[...]
        for j in range(0, d, BLOCK3):
            e = min(j + BLOCK3, d)
            part[:, j:e] = jnp.dot(lhs, w2o[:, j:e], preferred_element_type=F32).astype(BF16)
        d2d_copy(t).start()

        @pl.when(t >= 1)
        def _():
            s2(t - 1)

        @pl.when(t >= 3)
        def _():
            s4(t - 3)

        @pl.when(t >= 5)
        def _():
            s6(t - 5)

        @pl.when(t >= 4)
        def _():
            s5(t - 4)

    v_copy(in13, early - in13, 1).start()
    residual(n - 2)
    s1_last(n - 1)
    s3(n - 2)
    s2_last(n - 1)
    s4(n - 3)
    s6(n - 5)
    s5(n - 4)
    residual(n - 1)
    s3_last(n - 1)
    s4(n - 2)
    s6(n - 4)
    s5(n - 3)
    s4_last(n - 1)
    s6(n - 3)
    s5(n - 2)
    s6(n - 2)
    s5(n - 1)
    late = range(early, in_vmem)
    for i, j in enumerate(late):
        v_copy(j, 1, 2 + i).start()
    s6(n - 1)
    v_copy(0, in13, 0).wait()
    v_copy(in13, early - in13, 1).wait()
    for i, j in enumerate(late):
        v_copy(j, 1, 2 + i).wait()


def vmem_steps(n, d, dq, ff):
    in13 = d // TOK
    return in13, min(in13 + (dq + ff) // TOK, n - 1)


def finish(n, in_vmem, y, wbuf, out, buf, sem):
    loads = [pltpu.make_async_copy(y.at[pl.ds(j * TOK, TOK)], buf.at[j - in_vmem], sem.at[j]) for j in range(in_vmem, n)]
    stores = [pltpu.make_async_copy(wbuf.at[pl.ds(j * TOK, TOK)] if j < in_vmem else buf.at[j - in_vmem],
                                    out.at[pl.ds(j * TOK, TOK)], sem.at[n + j]) for j in range(n)]
    for cpy in loads + stores[:in_vmem]:
        cpy.start()
    for load, store in zip(loads, stores[in_vmem:]):
        load.wait()
        store.start()
    for cpy in stores:
        cpy.wait()


def solution(mesh):
    n_tp = mesh.shape["tp"]

    def local(x, gamma, beta, wq, wkv, wo, w1, w3, w2):
        b, s, d = x.shape
        dq, dh, ff = wq.shape[1], wkv.shape[1] // 2, w1.shape[1]
        n = b * s // TOK
        half = TOK // 2
        blk = half // (n_tp // 2)
        in13, in_vmem = vmem_steps(n, d, dq, ff)
        assert 2 * ff == d and in13 <= n - 6 and in_vmem > n - 5 and n_tp == 8
        dma = pltpu.SemaphoreType.DMA
        hbm = pl.BlockSpec(memory_space=pl.ANY)
        vmem = pl.BlockSpec(memory_space=pltpu.VMEM)
        y, wbuf = pl.pallas_call(
            functools.partial(kernel, n_tp, s),
            out_shape=(jax.ShapeDtypeStruct((b * s, d), BF16), pltpu.VMEM((d + dq + ff, d), BF16)),
            in_specs=[hbm, vmem, vmem] + [hbm] * 6,
            out_specs=(hbm, vmem),
            scratch_shapes=[
                pltpu.VMEM((2, d), F32),
                pltpu.VMEM((d, dq + dh), BF16),
                pltpu.VMEM((half, d), BF16),
                pltpu.VMEM((half, d), BF16),
                pltpu.VMEM((TOK, d), BF16),
                pltpu.VMEM((2, s, dh), BF16),
                pltpu.VMEM((TOK, dq + ff), BF16),
                pltpu.VMEM((TOK, d), BF16),
                pltpu.VMEM((3, half, d), BF16),
                pltpu.VMEM((3, blk, d), BF16),
                pltpu.VMEM((3, 2, blk, d), BF16),
                pltpu.VMEM((blk, d), BF16),
                dma((6,)), dma, dma, dma, dma, pltpu.SemaphoreType.REGULAR, dma, dma,
                dma((3,)), dma((3,)), dma((3,)), dma((3,)), dma((3,)),
                dma, dma((4,)), dma((3,)), dma((3,)), dma((3,)), dma((3,)), dma((7,)),
            ],
            compiler_params=pltpu.CompilerParams(collective_id=0, has_side_effects=True, vmem_limit_bytes=VMEM_LIMIT),
        )(x.reshape(b * s, d), gamma, beta, wq, wkv, wo, w1, w3, w2)
        out = pl.pallas_call(
            functools.partial(finish, n, in_vmem),
            out_shape=jax.ShapeDtypeStruct((b * s, d), BF16),
            in_specs=[hbm, vmem],
            out_specs=hbm,
            scratch_shapes=[pltpu.VMEM((n - in_vmem, TOK, d), BF16), dma((2 * n,))],
            compiler_params=pltpu.CompilerParams(vmem_limit_bytes=8 * 1024 * 1024),
        )(y, wbuf)
        return out.reshape(b, s, d)

    return jax.shard_map(local, mesh=mesh,
                         in_specs=(P('dp', None, None), P(), P(), P(None, 'tp'), P(), P('tp', None),
                                   P(None, 'tp'), P(None, 'tp'), P('tp', None)),
                         out_specs=P('dp', None, None), check_vma=False)
```

```python
import functools

import jax
import jax.numpy as jnp
from jax import lax
from jax.experimental import pallas as pl
from jax.experimental.pallas import tpu as pltpu
from jax.sharding import PartitionSpec as P

EPS = 1e-5
MESH = pl.DeviceIdType.MESH
TOK = 256
LOG2E = 1.4426950408889634
F32 = jnp.float32
BF16 = jnp.bfloat16
VMEM_LIMIT = 24_800_000
BLOCK3 = 512


def kernel(n_tp, seq,
           x, gamma, beta, wq, wkv, wo, w1, w3, w2,
           y, wbuf,
           gb, wqkv, xin, lnst, ln, kv, act, part, pbuf, r1, r2, ybuf,
           wsem, xsem, xrsem, lns, lnr, free, kvs, kvr, ds_, dr_, us, ur, s1r,
           ys, yr, fs, fr, gs, gr, vsem):
    d = x.shape[1]
    n = x.shape[0] // TOK
    per_seq = seq // TOK
    dq = wq.shape[1]
    dh = wkv.shape[1] // 2
    ff = w1.shape[1]
    nh = dq // dh
    half = TOK // 2
    chips = n_tp // 2
    blk = half // chips
    dm = d // 2
    w13, w2o = wbuf.at[pl.ds(0, d)], wbuf.at[pl.ds(d, dq + ff)]

    me = lax.axis_index("tp")
    h = lax.rem(me, 2)
    c = me // 2
    cp = lax.rem(c + 1, chips)
    cm = lax.rem(c + chips - 1, chips)
    co = lax.rem(c + 2, chips)
    plus, minus, partner = cp * 2 + h, cm * 2 + h, c * 2 + 1 - h
    ca, cb = pl.ds(0, dm), pl.ds(dm, dm)

    def rcopy(src, dst, ssem, rsem, dev):
        return pltpu.make_async_remote_copy(src_ref=src, dst_ref=dst, send_sem=ssem, recv_sem=rsem,
                                            device_id={"tp": dev}, device_id_type=MESH)

    def own(ref):
        return ref.at[pl.ds(pl.multiple_of(h * half, half), half)]

    def rows_of(k):
        return pl.ds(pl.multiple_of(k * blk, blk), blk)

    def yrows(j, k):
        return pl.ds(pl.multiple_of(j * TOK + h * half + k * blk, blk), blk)

    def x_copy(j):
        return pltpu.make_async_copy(x.at[pl.ds(pl.multiple_of(j * TOK + h * half, half), half)], xin, xsem)

    def xres_copy(j):
        return pltpu.make_async_copy(x.at[yrows(j, c)], ybuf, xrsem)

    tiles = ff // min(256, ff)
    first_tiles = min(3, tiles - 1)
    cut = first_tiles * min(256, ff)

    def w_group(pairs, first_sem):
        return tuple(pltpu.make_async_copy(src, dst, wsem.at[first_sem + i]) for i, (src, dst) in enumerate(pairs))

    w_first = w_group(
        [(wq, wqkv.at[:, pl.ds(0, dq)]), (wkv.at[:, pl.ds(pl.multiple_of(h * dh, dh), dh)], wqkv.at[:, pl.ds(dq, dh)])]
        + ([(w1.at[:, pl.ds(0, cut)], w13.at[:, pl.ds(0, cut)]), (w3.at[:, pl.ds(0, cut)], w13.at[:, pl.ds(ff, cut)])]
           if cut else []), 0)
    w_second = w_group([(w1.at[:, pl.ds(cut, ff - cut)], w13.at[:, pl.ds(cut, ff - cut)]),
                        (w3.at[:, pl.ds(cut, ff - cut)], w13.at[:, pl.ds(ff + cut, ff - cut)])], 4)
    w_third = w_group([(wo, w2o.at[pl.ds(0, dq)]), (w2, w2o.at[pl.ds(dq, ff)])], 6)

    def layer_norm(r0, r1):
        for r in range(r0, r1, 16):
            xf = xin[r:r + 16, :].astype(F32)
            mu = jnp.mean(xf, axis=-1, keepdims=True)
            xc = xf - mu
            var = jnp.mean(jnp.square(xc), axis=-1, keepdims=True)
            lnst[r:r + 16, :] = (xc * lax.rsqrt(var + EPS) * gb[0:1, :] + gb[1:2, :]).astype(BF16)

    def ln_local():
        ln[pl.ds(pl.multiple_of(h * half, half), half), :] = lnst[...]

    def ln_copy():
        return rcopy(lnst, own(ln), lns, lnr, partner)

    def kv_copy(t):
        view = kv.at[h, pl.ds(pl.multiple_of(lax.rem(t, per_seq) * TOK, TOK), TOK)]
        return rcopy(view, view, kvs, kvr, partner)

    def got(sem, k):
        view = part.at[pl.ds(0, k * blk)]
        rcopy(view, view, sem, sem, partner).wait_recv()

    def sent(sem, k):
        view = part.at[pl.ds(0, k * blk)]
        rcopy(view, view, sem, sem, partner).wait_send()

    def d2d_copy(j):
        p = lax.rem(j, 3)
        return rcopy(part.at[pl.ds(pl.multiple_of((1 - h) * half, half), half)], pbuf.at[p], ds_.at[p], dr_.at[p], partner)

    def ways(j):
        even = lax.rem(j, 2) == 0
        pick = lambda u, v: jnp.where(even, u, v)
        return pick(plus, minus), pick(minus, plus), pick(cp, cm), pick(cm, cp), pick(0, 1), pick(1, 0)

    def s1_add(j):
        p = lax.rem(j, 3)
        got(dr_.at[p], chips)
        sent(ds_.at[p], chips)

        @pl.loop(0, half // 32)
        def _(i):
            mine = part[pl.ds(pl.multiple_of(h * half + i * 32, 32), 32), :]
            rr = pl.ds(pl.multiple_of(i * 32, 32), 32)
            pbuf[p, rr, :] = mine + pbuf[p, rr, :]

    def s1(j):
        p = lax.rem(j, 3)
        ahead, behind, _, k_behind, _, i_behind = ways(j)
        s1_add(j)
        rcopy(pbuf.at[p, rows_of(co)], r1.at[p], us.at[p], s1r.at[p], ahead).start()
        rcopy(pbuf.at[p, rows_of(k_behind)], r2.at[p, i_behind], us.at[p], ur.at[p], behind).start()

    def s2(j):
        p = lax.rem(j, 3)
        ahead, _, k_ahead, _, i_ahead, _ = ways(j)
        got(s1r.at[p], 1)
        pbuf[p, rows_of(k_ahead), :] = pbuf[p, rows_of(k_ahead), :] + r1[p]
        rcopy(pbuf.at[p, rows_of(k_ahead)], r2.at[p, i_ahead], us.at[p], ur.at[p], ahead).start()

    def residual(j):
        @pl.when(j >= 1)
        def _():
            sent(ys, 3)

        xres_copy(j).start()

    def s3_sum(j):
        p = lax.rem(j, 3)
        got(ur.at[p], 2)
        xres_copy(j).wait()
        ybuf[...] = (ybuf[...].astype(F32) + ((pbuf[p, rows_of(c), :].astype(F32) + r2[p, 0].astype(F32))
                                          + r2[p, 1].astype(F32))).astype(BF16)

    def y_local(j):
        pltpu.make_async_copy(ybuf, y.at[yrows(j, c)], ys).start()

    def s3(j):
        p = lax.rem(j, 3)
        s3_sum(j)
        for dev in (plus, minus):
            rcopy(ybuf, y.at[yrows(j, c)], ys, yr.at[p], dev).start()
        y_local(j)
        sent(us.at[p], 3)

    def s4(j):
        p = lax.rem(j, 3)
        _, behind, k_ahead, _, _, _ = ways(j)
        got(yr.at[p], 2)
        view = y.at[yrows(j, k_ahead)]
        rcopy(view, view, fs.at[p], fr.at[p], behind).start()

    def s5(j):
        p = lax.rem(j, 3)
        got(fr.at[p], 1)
        view = y.at[pl.ds(pl.multiple_of(j * TOK + h * half, half), half)]
        rcopy(view, view, gs.at[p], gr.at[p], partner).start()
        sent(fs.at[p], 1)

    def g_last(j, k):
        view = y.at[yrows(j, k)]
        rcopy(view, view, gs.at[3], gr.at[3], partner).start()

    def s5_last(j):
        p = lax.rem(j, 3)
        got(fr.at[p], 1)
        g_last(j, co)
        sent(fs.at[p], 1)

    def s6(j):
        p = lax.rem(j, 3)
        got(gr.at[p], chips)
        sent(gs.at[p], chips)

    def s1_last(j):
        p = lax.rem(j, 3)
        s1_add(j)
        rcopy(pbuf.at[p, rows_of(co), ca], r1.at[p, :, ca], us.at[p], s1r.at[p], plus).start()
        rcopy(pbuf.at[p, rows_of(co), cb], r1.at[p, :, cb], us.at[p], s1r.at[p], minus).start()
        rcopy(pbuf.at[p, rows_of(cp), cb], r2.at[p, 0, :, cb], us.at[p], ur.at[p], plus).start()
        rcopy(pbuf.at[p, rows_of(cm), ca], r2.at[p, 1, :, ca], us.at[p], ur.at[p], minus).start()

    def s2_last(j):
        p = lax.rem(j, 3)
        got(s1r.at[p], 1)
        pbuf[p, rows_of(cp), :dm] = pbuf[p, rows_of(cp), :dm] + r1[p, :, :dm]
        pbuf[p, rows_of(cm), dm:] = pbuf[p, rows_of(cm), dm:] + r1[p, :, dm:]
        rcopy(pbuf.at[p, rows_of(cp), ca], r2.at[p, 0, :, ca], us.at[p], ur.at[p], plus).start()
        rcopy(pbuf.at[p, rows_of(cm), cb], r2.at[p, 1, :, cb], us.at[p], ur.at[p], minus).start()

    def s3_last(j):
        p = lax.rem(j, 3)
        s3_sum(j)
        for cols, sem, dev in ((ca, yr.at[p], plus), (cb, yr.at[p], minus), (cb, yr.at[3], plus), (ca, yr.at[3], minus)):
            rcopy(ybuf.at[:, cols], y.at[yrows(j, c), cols], ys, sem, dev).start()
        y_local(j)
        sent(us.at[p], 3)

    def s4_last(j):
        p = lax.rem(j, 3)
        got(yr.at[p], 1)
        for k, cols, dev in ((cm, ca, plus), (cp, cb, minus)):
            view = y.at[yrows(j, k), cols]
            rcopy(view, view, fs.at[p], fr.at[p], dev).start()
        got(yr.at[3], 1)
        sent(ys, 3)
        for k in (c, cm, cp):
            g_last(j, k)

    def hidden(j0, j1):
        lhs = ln[...]
        tile = min(256, ff)
        for j in range(j0 * tile, j1 * tile, tile):
            g = jnp.dot(lhs, w13[:, j:j + tile], preferred_element_type=F32)
            u = jnp.dot(lhs, w13[:, ff + j:ff + j + tile], preferred_element_type=F32)
            act[:, dq + j:dq + j + tile] = (jax.nn.silu(g) * u).astype(BF16)

    def attend(t, blocks):
        keys = blocks * TOK
        k = kv[0, :keys, :]
        v = kv[1, :keys, :]
        open_ = max(keys - 2 * TOK, 0)
        qi = lax.broadcasted_iota(jnp.int32, (TOK, keys - open_), 0)
        ki = lax.broadcasted_iota(jnp.int32, (TOK, keys - open_), 1)
        seen = ki + open_ <= qi + lax.rem(t, per_seq) * TOK
        rest = list(range(first_tiles, tiles))
        for a in range(nh):
            q = act[:, a * dh:(a + 1) * dh]
            sc = lax.dot_general(q, k, (((1,), (1,)), ((), ())), preferred_element_type=F32)
            sc = sc * (dh ** -0.5 * LOG2E)
            if rest:
                j = rest.pop(0)
                hidden(j, j + 1)
            last = jnp.where(seen, sc[:, open_:], -1e30)
            sc = last if open_ == 0 else jnp.concatenate([sc[:, :open_], last], axis=1)
            p = jnp.exp2(sc - jnp.max(sc, axis=-1, keepdims=True))
            p = (p * (1.0 / jnp.sum(p, axis=-1, keepdims=True))).astype(BF16)
            if rest and a + 1 < nh:
                j = rest.pop(0)
                hidden(j, j + 1)
            act[:, a * dh:(a + 1) * dh] = jnp.dot(p, v, preferred_element_type=F32).astype(BF16)
        for j in rest:
            hidden(j, j + 1)

    in13, in_vmem = vmem_steps(n, d, dq, ff)
    early = n - 5

    def v_copy(j, steps, i):
        rows = pl.ds(j * TOK, steps * TOK)
        return pltpu.make_async_copy(y.at[rows], wbuf.at[rows], vsem.at[i])

    barrier = pltpu.get_barrier_semaphore()
    for dev in (partner, plus, minus):
        pl.semaphore_signal(barrier, inc=1, device_id={"tp": dev}, device_id_type=MESH)
    x_copy(0).start()
    for cpy in w_first:
        cpy.start()
    gb[0:1, :] = gamma[...][None, :]
    gb[1:2, :] = beta[...][None, :]
    pl.semaphore_wait(barrier, 3)
    x_copy(0).wait()
    layer_norm(0, half)
    ln_local()
    ln_copy().start()
    x_copy(1).start()
    for cpy in w_second:
        cpy.start()

    @pl.loop(0, n)
    def _(t):
        ln_copy().wait_recv()
        ln_copy().wait_send()

        @pl.when(t == 0)
        def _():
            for cpy in w_first:
                cpy.wait()

        @pl.when(t + 1 < n)
        def _():
            x_copy(t + 1).wait()

        pos = lax.rem(t, per_seq)

        @pl.when(lax.rem(pos, 2) == 0)
        def _():
            kv[1, pl.ds(pl.multiple_of((pos + 1) * TOK, TOK), TOK), :] = jnp.zeros((TOK, dh), BF16)

        act[:, :dq] = jnp.dot(ln[...], wqkv[:, :dq], preferred_element_type=F32).astype(BF16)
        for r in range(0, TOK, half):
            kv[h, pl.ds(pl.multiple_of(pos * TOK + r, half), half), :] = jnp.dot(
                ln[r:r + half, :], wqkv[:, dq:], preferred_element_type=F32).astype(BF16)
        kv_copy(t).start()
        step = half // max(first_tiles, 1) // 16 * 16
        for i in range(first_tiles):
            layer_norm(i * step, (i + 1) * step)
            hidden(i, i + 1)
        layer_norm(first_tiles * step, half)

        @pl.when(t + 2 < n)
        def _():
            x_copy(t + 2).start()

        @pl.when(t >= 1)
        def _():
            s1(t - 1)

        @pl.when(t >= 2)
        def _():
            residual(t - 2)

        @pl.when(t == 0)
        def _():
            for cpy in w_third:
                cpy.start()
            for cpy in w_second:
                cpy.wait()

        kv_copy(t).wait_recv()
        kv_copy(t).wait_send()
        for b in range(0, per_seq, 2):
            pl.when((pos == b) | (pos == b + 1))(functools.partial(attend, t, b + 2))
        pl.semaphore_signal(free, inc=1, device_id={"tp": partner}, device_id_type=MESH)

        @pl.when(t >= 2)
        def _():
            s3(t - 2)

        pl.semaphore_wait(free, 1)

        @pl.when(t == 0)
        def _():
            for cpy in w_third:
                cpy.wait()

        @pl.when(t == n - 1)
        def _():
            v_copy(0, in13, 0).start()

        @pl.when(t + 1 < n)
        def _():
            ln_copy().start()

        ln_local()
        lhs = act[...]
        for j in range(0, d, BLOCK3):
            e = min(j + BLOCK3, d)
            part[:, j:e] = jnp.dot(lhs, w2o[:, j:e], preferred_element_type=F32).astype(BF16)
        d2d_copy(t).start()

        @pl.when(t >= 1)
        def _():
            s2(t - 1)

        @pl.when(t >= 3)
        def _():
            s4(t - 3)

        @pl.when(t >= 5)
        def _():
            s6(t - 5)

        @pl.when(t >= 4)
        def _():
            s5(t - 4)

    v_copy(in13, early - in13, 1).start()
    residual(n - 2)
    s1_last(n - 1)
    s3(n - 2)
    s2_last(n - 1)
    s6(n - 5)
    v_copy(n - 5, 1, 2).start()
    s4(n - 3)
    residual(n - 1)
    s4(n - 2)
    s5(n - 4)
    s3_last(n - 1)
    s6(n - 4)
    v_copy(n - 4, 1, 3).start()
    s5(n - 3)
    s4_last(n - 1)
    s5(n - 2)
    s6(n - 3)
    v_copy(n - 3, 1, 4).start()
    s6(n - 2)
    v_copy(n - 2, 1, 5).start()
    s5_last(n - 1)
    got(gr.at[3], chips)
    sent(gs.at[3], chips)
    v_copy(0, in13, 0).wait()
    v_copy(in13, early - in13, 1).wait()
    for i, j in enumerate(range(n - 5, n - 1)):
        v_copy(j, 1, 2 + i).wait()


def vmem_steps(n, d, dq, ff):
    in13 = d // TOK
    return in13, min(in13 + (dq + ff) // TOK, n - 1)


def finish(n, in_vmem, y, wbuf, out, buf, sem):
    loads = [pltpu.make_async_copy(y.at[pl.ds(j * TOK, TOK)], buf.at[j - in_vmem], sem.at[j]) for j in range(in_vmem, n)]
    stores = [pltpu.make_async_copy(wbuf.at[pl.ds(j * TOK, TOK)] if j < in_vmem else buf.at[j - in_vmem],
                                    out.at[pl.ds(j * TOK, TOK)], sem.at[n + j]) for j in range(n)]
    for cpy in loads + stores[:in_vmem]:
        cpy.start()
    for load, store in zip(loads, stores[in_vmem:]):
        load.wait()
        store.start()
    for cpy in stores:
        cpy.wait()


def solution(mesh):
    n_tp = mesh.shape["tp"]

    def local(x, gamma, beta, wq, wkv, wo, w1, w3, w2):
        b, s, d = x.shape
        dq, dh, ff = wq.shape[1], wkv.shape[1] // 2, w1.shape[1]
        n = b * s // TOK
        half = TOK // 2
        blk = half // (n_tp // 2)
        in13, in_vmem = vmem_steps(n, d, dq, ff)
        assert 2 * ff == d and in13 <= n - 6 and in_vmem == n - 1 and n_tp == 8
        dma = pltpu.SemaphoreType.DMA
        hbm = pl.BlockSpec(memory_space=pl.ANY)
        vmem = pl.BlockSpec(memory_space=pltpu.VMEM)
        y, wbuf = pl.pallas_call(
            functools.partial(kernel, n_tp, s),
            out_shape=(jax.ShapeDtypeStruct((b * s, d), BF16), pltpu.VMEM((d + dq + ff, d), BF16)),
            in_specs=[hbm, vmem, vmem] + [hbm] * 6,
            out_specs=(hbm, vmem),
            scratch_shapes=[
                pltpu.VMEM((2, d), F32),
                pltpu.VMEM((d, dq + dh), BF16),
                pltpu.VMEM((half, d), BF16),
                pltpu.VMEM((half, d), BF16),
                pltpu.VMEM((TOK, d), BF16),
                pltpu.VMEM((2, s, dh), BF16),
                pltpu.VMEM((TOK, dq + ff), BF16),
                pltpu.VMEM((TOK, d), BF16),
                pltpu.VMEM((3, half, d), BF16),
                pltpu.VMEM((3, blk, d), BF16),
                pltpu.VMEM((3, 2, blk, d), BF16),
                pltpu.VMEM((blk, d), BF16),
                dma((8,)), dma, dma, dma, dma, pltpu.SemaphoreType.REGULAR, dma, dma,
                dma((3,)), dma((3,)), dma((3,)), dma((3,)), dma((3,)),
                dma, dma((4,)), dma((3,)), dma((3,)), dma((4,)), dma((4,)), dma((6,)),
            ],
            compiler_params=pltpu.CompilerParams(collective_id=0, has_side_effects=True, vmem_limit_bytes=VMEM_LIMIT),
        )(x.reshape(b * s, d), gamma, beta, wq, wkv, wo, w1, w3, w2)
        out = pl.pallas_call(
            functools.partial(finish, n, in_vmem),
            out_shape=jax.ShapeDtypeStruct((b * s, d), BF16),
            in_specs=[hbm, vmem],
            out_specs=hbm,
            scratch_shapes=[pltpu.VMEM((n - in_vmem, TOK, d), BF16), dma((2 * n,))],
            compiler_params=pltpu.CompilerParams(vmem_limit_bytes=8 * 1024 * 1024),
        )(y, wbuf)
        return out.reshape(b, s, d)

    return jax.shard_map(local, mesh=mesh,
                         in_specs=(P('dp', None, None), P(), P(), P(None, 'tp'), P(), P('tp', None),
                                   P(None, 'tp'), P(None, 'tp'), P('tp', None)),
                         out_specs=P('dp', None, None), check_vma=False)
```

```python
import functools

import jax
import jax.numpy as jnp
from jax import lax
from jax.experimental import pallas as pl
from jax.experimental.pallas import tpu as pltpu
from jax.sharding import PartitionSpec as P

EPS = 1e-5
MESH = pl.DeviceIdType.MESH
TOK = 256
LOG2E = 1.4426950408889634
F32 = jnp.float32
BF16 = jnp.bfloat16
VMEM_LIMIT = 22_980_000
BLOCK3 = 512


def kernel(n_tp, seq,
           x, gamma, beta, wq, wkv, wo, w1, w3, w2,
           y, wbuf,
           gb, wqkv, xin, lnst, ln, kv, act, pbuf, r1, r2, ybuf,
           wsem, xsem, xrsem, lns, lnr, free, kvs, kvr, ds_, dr_, us, ur, s1r,
           ys, yr, fs, fr, gs, gr, vsem):
    d = x.shape[1]
    n = x.shape[0] // TOK
    per_seq = seq // TOK
    dq = wq.shape[1]
    dh = wkv.shape[1] // 2
    ff = w1.shape[1]
    nh = dq // dh
    half = TOK // 2
    chips = n_tp // 2
    blk = half // chips
    dm = d // 2
    w13, w2o = wbuf.at[pl.ds(0, d)], wbuf.at[pl.ds(d, dq + ff)]
    part = wbuf.at[pl.ds(d + dq + ff, TOK)]

    me = lax.axis_index("tp")
    h = lax.rem(me, 2)
    c = me // 2
    cp = lax.rem(c + 1, chips)
    cm = lax.rem(c + chips - 1, chips)
    co = lax.rem(c + 2, chips)
    plus, minus, partner = cp * 2 + h, cm * 2 + h, c * 2 + 1 - h
    ca, cb = pl.ds(0, dm), pl.ds(dm, dm)

    def rcopy(src, dst, ssem, rsem, dev):
        return pltpu.make_async_remote_copy(src_ref=src, dst_ref=dst, send_sem=ssem, recv_sem=rsem,
                                            device_id={"tp": dev}, device_id_type=MESH)

    def own(ref):
        return ref.at[pl.ds(pl.multiple_of(h * half, half), half)]

    def rows_of(k):
        return pl.ds(pl.multiple_of(k * blk, blk), blk)

    def yrows(j, k):
        return pl.ds(pl.multiple_of(j * TOK + h * half + k * blk, blk), blk)

    def x_copy(j):
        return pltpu.make_async_copy(x.at[pl.ds(pl.multiple_of(j * TOK + h * half, half), half)], xin, xsem)

    def xres_copy(j):
        return pltpu.make_async_copy(x.at[yrows(j, c)], ybuf, xrsem)

    tiles = ff // min(256, ff)
    first_tiles = min(3, tiles - 1)
    cut = first_tiles * min(256, ff)

    def w_group(pairs, first_sem):
        return tuple(pltpu.make_async_copy(src, dst, wsem.at[first_sem + i]) for i, (src, dst) in enumerate(pairs))

    w_first = w_group(
        [(wq, wqkv.at[:, pl.ds(0, dq)]), (wkv.at[:, pl.ds(pl.multiple_of(h * dh, dh), dh)], wqkv.at[:, pl.ds(dq, dh)])]
        + ([(w1.at[:, pl.ds(0, cut)], w13.at[:, pl.ds(0, cut)]), (w3.at[:, pl.ds(0, cut)], w13.at[:, pl.ds(ff, cut)])]
           if cut else []), 0)
    w_second = w_group([(w1.at[:, pl.ds(cut, ff - cut)], w13.at[:, pl.ds(cut, ff - cut)]),
                        (w3.at[:, pl.ds(cut, ff - cut)], w13.at[:, pl.ds(ff + cut, ff - cut)])], 4)
    w_third = w_group([(wo, w2o.at[pl.ds(0, dq)]), (w2, w2o.at[pl.ds(dq, ff)])], 6)

    def layer_norm(r0, r1):
        for r in range(r0, r1, 16):
            xf = xin[r:r + 16, :].astype(F32)
            mu = jnp.mean(xf, axis=-1, keepdims=True)
            xc = xf - mu
            var = jnp.mean(jnp.square(xc), axis=-1, keepdims=True)
            lnst[r:r + 16, :] = (xc * lax.rsqrt(var + EPS) * gb[0:1, :] + gb[1:2, :]).astype(BF16)

    def ln_local():
        ln[pl.ds(pl.multiple_of(h * half, half), half), :] = lnst[...]

    def ln_copy():
        return rcopy(lnst, own(ln), lns, lnr, partner)

    def kv_copy(t):
        view = kv.at[h, pl.ds(pl.multiple_of(lax.rem(t, per_seq) * TOK, TOK), TOK)]
        return rcopy(view, view, kvs, kvr, partner)

    def got(sem, k):
        view = part.at[pl.ds(0, k * blk)]
        rcopy(view, view, sem, sem, partner).wait_recv()

    def sent(sem, k):
        view = part.at[pl.ds(0, k * blk)]
        rcopy(view, view, sem, sem, partner).wait_send()

    def d2d_copy(j):
        p = lax.rem(j, 3)
        return rcopy(part.at[pl.ds(pl.multiple_of((1 - h) * half, half), half)], pbuf.at[p], ds_.at[p], dr_.at[p], partner)

    def ways(j):
        even = lax.rem(j, 2) == 0
        pick = lambda u, v: jnp.where(even, u, v)
        return pick(plus, minus), pick(minus, plus), pick(cp, cm), pick(cm, cp), pick(0, 1), pick(1, 0)

    def s1_add(j):
        p = lax.rem(j, 3)
        got(dr_.at[p], chips)
        sent(ds_.at[p], chips)

        @pl.loop(0, half // 32)
        def _(i):
            mine = part[pl.ds(pl.multiple_of(h * half + i * 32, 32), 32), :]
            rr = pl.ds(pl.multiple_of(i * 32, 32), 32)
            pbuf[p, rr, :] = mine + pbuf[p, rr, :]

    def s1(j):
        p = lax.rem(j, 3)
        ahead, behind, _, k_behind, _, i_behind = ways(j)
        s1_add(j)
        rcopy(pbuf.at[p, rows_of(co)], r1.at[p], us.at[p], s1r.at[p], ahead).start()
        rcopy(pbuf.at[p, rows_of(k_behind)], r2.at[p, i_behind], us.at[p], ur.at[p], behind).start()

    def s2(j):
        p = lax.rem(j, 3)
        ahead, _, k_ahead, _, i_ahead, _ = ways(j)
        got(s1r.at[p], 1)
        pbuf[p, rows_of(k_ahead), :] = pbuf[p, rows_of(k_ahead), :] + r1[p]
        rcopy(pbuf.at[p, rows_of(k_ahead)], r2.at[p, i_ahead], us.at[p], ur.at[p], ahead).start()

    def residual(j):
        @pl.when(j >= 1)
        def _():
            sent(ys, 3)

        xres_copy(j).start()

    def residual_on(j):
        sent(ys, 3)
        xres_copy(j).start()

    def s3_sum(j):
        p = lax.rem(j, 3)
        got(ur.at[p], 2)
        xres_copy(j).wait()
        ybuf[...] = (ybuf[...].astype(F32) + ((pbuf[p, rows_of(c), :].astype(F32) + r2[p, 0].astype(F32))
                                          + r2[p, 1].astype(F32))).astype(BF16)

    def y_local(j):
        pltpu.make_async_copy(ybuf, y.at[yrows(j, c)], ys).start()

    def s3(j):
        p = lax.rem(j, 3)
        s3_sum(j)
        for dev in (plus, minus):
            rcopy(ybuf, y.at[yrows(j, c)], ys, yr.at[p], dev).start()
        y_local(j)
        sent(us.at[p], 3)

    def s4(j):
        p = lax.rem(j, 3)
        _, behind, k_ahead, _, _, _ = ways(j)
        got(yr.at[p], 2)
        view = y.at[yrows(j, k_ahead)]
        rcopy(view, view, fs.at[p], fr.at[p], behind).start()

    def s5(j):
        p = lax.rem(j, 3)
        got(fr.at[p], 1)
        view = y.at[pl.ds(pl.multiple_of(j * TOK + h * half, half), half)]
        rcopy(view, view, gs.at[p], gr.at[p], partner).start()
        sent(fs.at[p], 1)

    def s6(j):
        p = lax.rem(j, 3)
        got(gr.at[p], chips)
        sent(gs.at[p], chips)

    def s1_last(j):
        p = lax.rem(j, 3)
        s1_add(j)
        rcopy(pbuf.at[p, rows_of(co), ca], r1.at[p, :, ca], us.at[p], s1r.at[p], plus).start()
        rcopy(pbuf.at[p, rows_of(co), cb], r1.at[p, :, cb], us.at[p], s1r.at[p], minus).start()
        rcopy(pbuf.at[p, rows_of(cp), cb], r2.at[p, 0, :, cb], us.at[p], ur.at[p], plus).start()
        rcopy(pbuf.at[p, rows_of(cm), ca], r2.at[p, 1, :, ca], us.at[p], ur.at[p], minus).start()

    def s2_last(j):
        p = lax.rem(j, 3)
        got(s1r.at[p], 1)
        pbuf[p, rows_of(cp), :dm] = pbuf[p, rows_of(cp), :dm] + r1[p, :, :dm]
        pbuf[p, rows_of(cm), dm:] = pbuf[p, rows_of(cm), dm:] + r1[p, :, dm:]
        rcopy(pbuf.at[p, rows_of(cp), ca], r2.at[p, 0, :, ca], us.at[p], ur.at[p], plus).start()
        rcopy(pbuf.at[p, rows_of(cm), cb], r2.at[p, 1, :, cb], us.at[p], ur.at[p], minus).start()

    def last_rows(k):
        return pl.ds(pl.multiple_of(h * half + k * blk, blk), blk)

    def s3_last(j):
        p = lax.rem(j, 3)
        s3_sum(j)
        part[last_rows(c), :] = ybuf[...]
        for cols, sem, dev in ((ca, yr.at[p], plus), (cb, yr.at[p], minus), (cb, yr.at[3], plus), (ca, yr.at[3], minus)):
            rcopy(ybuf.at[:, cols], part.at[last_rows(c), cols], ys, sem, dev).start()
        pl.semaphore_wait(free, 1)
        g_last(c)
        sent(us.at[p], 3)

    def s4_last(j):
        p = lax.rem(j, 3)
        got(yr.at[p], 1)
        for k, cols, dev in ((cm, ca, plus), (cp, cb, minus)):
            view = part.at[last_rows(k), cols]
            rcopy(view, view, fs.at[p], fr.at[p], dev).start()
        got(yr.at[3], 1)
        for k in (cm, cp):
            g_last(k)
        sent(ys, 2)

    def g_last(k):
        view = part.at[last_rows(k)]
        rcopy(view, view, gs.at[3], gr.at[3], partner).start()

    def s5_last(j):
        p = lax.rem(j, 3)
        got(fr.at[p], 1)
        g_last(co)
        sent(fs.at[p], 1)

    def hidden(j0, j1):
        lhs = ln[...]
        tile = min(256, ff)
        for j in range(j0 * tile, j1 * tile, tile):
            g = jnp.dot(lhs, w13[:, j:j + tile], preferred_element_type=F32)
            u = jnp.dot(lhs, w13[:, ff + j:ff + j + tile], preferred_element_type=F32)
            act[:, dq + j:dq + j + tile] = (jax.nn.silu(g) * u).astype(BF16)

    def attend(t, blocks):
        keys = blocks * TOK
        k = kv[0, :keys, :]
        v = kv[1, :keys, :]
        open_ = max(keys - 2 * TOK, 0)
        qi = lax.broadcasted_iota(jnp.int32, (TOK, keys - open_), 0)
        ki = lax.broadcasted_iota(jnp.int32, (TOK, keys - open_), 1)
        seen = ki + open_ <= qi + lax.rem(t, per_seq) * TOK
        rest = list(range(first_tiles, tiles))

        def tile(count=1):
            for _ in range(count):
                if rest:
                    j = rest.pop(0)
                    hidden(j, j + 1)

        def scores(a):
            q = act[:, a * dh:(a + 1) * dh]
            sc = lax.dot_general(q, k, (((1,), (1,)), ((), ())), preferred_element_type=F32)
            sc = sc * (dh ** -0.5 * LOG2E)
            last = jnp.where(seen, sc[:, open_:], -1e30)
            return last if open_ == 0 else jnp.concatenate([sc[:, :open_], last], axis=1)

        def weights(sc):
            p = jnp.exp2(sc - jnp.max(sc, axis=-1, keepdims=True))
            return (p * (1.0 / jnp.sum(p, axis=-1, keepdims=True))).astype(BF16)

        def values(a, p):
            act[:, a * dh:(a + 1) * dh] = jnp.dot(p, v, preferred_element_type=F32).astype(BF16)

        tile(1)
        for a in range(nh):
            sc = scores(a)
            tile(1)
            p = weights(sc)
            if a + 1 < nh:
                tile(1)
            values(a, p)
        tile(tiles)

    in13, early = d // TOK, n - 5

    def v_copy(j, steps, i):
        rows = pl.ds(j * TOK, steps * TOK)
        return pltpu.make_async_copy(y.at[rows], wbuf.at[rows], vsem.at[i])

    def stages(t, todo):
        full = max(lag for _, lag in todo)

        @pl.when(t >= full)
        def _():
            for stage, lag in todo:
                (residual_on if stage is residual else stage)(t - lag)

        @pl.when(t < full)
        def _():
            for stage, lag in todo:
                if lag < full:
                    pl.when(t >= lag)(functools.partial(stage, t - lag))

    barrier = pltpu.get_barrier_semaphore()
    for dev in (partner, plus, minus):
        pl.semaphore_signal(barrier, inc=1, device_id={"tp": dev}, device_id_type=MESH)
    x_copy(0).start()
    for cpy in w_first:
        cpy.start()
    gb[0:1, :] = gamma[...][None, :]
    gb[1:2, :] = beta[...][None, :]
    pl.semaphore_wait(barrier, 3)
    x_copy(0).wait()
    layer_norm(0, half)
    ln_local()
    ln_copy().start()
    x_copy(1).start()
    for cpy in w_second:
        cpy.start()

    @pl.loop(0, n)
    def _(t):
        ln_copy().wait_recv()
        ln_copy().wait_send()

        @pl.when(t == 0)
        def _():
            for cpy in w_first:
                cpy.wait()

        @pl.when(t + 1 < n)
        def _():
            x_copy(t + 1).wait()

        pos = lax.rem(t, per_seq)

        @pl.when(lax.rem(pos, 2) == 0)
        def _():
            kv[1, pl.ds(pl.multiple_of((pos + 1) * TOK, TOK), TOK), :] = jnp.zeros((TOK, dh), BF16)

        act[:, :dq] = jnp.dot(ln[...], wqkv[:, :dq], preferred_element_type=F32).astype(BF16)
        for r in range(0, TOK, half):
            kv[h, pl.ds(pl.multiple_of(pos * TOK + r, half), half), :] = jnp.dot(
                ln[r:r + half, :], wqkv[:, dq:], preferred_element_type=F32).astype(BF16)
        kv_copy(t).start()
        step = half // max(first_tiles, 1) // 16 * 16
        for i in range(first_tiles):
            layer_norm(i * step, (i + 1) * step)
            hidden(i, i + 1)
        layer_norm(first_tiles * step, half)

        @pl.when(t + 2 < n)
        def _():
            x_copy(t + 2).start()

        stages(t, ((s1, 1), (residual, 2), (s5, 5)))

        @pl.when(t == 0)
        def _():
            for cpy in w_third:
                cpy.start()
            for cpy in w_second:
                cpy.wait()

        kv_copy(t).wait_recv()
        kv_copy(t).wait_send()
        for b in range(0, per_seq, 2):
            pl.when((pos == b) | (pos == b + 1))(functools.partial(attend, t, b + 2))
        pl.semaphore_signal(free, inc=1, device_id={"tp": partner}, device_id_type=MESH)

        @pl.when(t >= 2)
        def _():
            s3(t - 2)

        pl.semaphore_wait(free, 1)

        @pl.when(t == 0)
        def _():
            for cpy in w_third:
                cpy.wait()

        @pl.when(t == n - 1)
        def _():
            v_copy(0, in13, 0).start()

        @pl.when(t + 1 < n)
        def _():
            ln_copy().start()

        ln_local()
        lhs = act[...]
        for j in range(0, d, BLOCK3):
            e = min(j + BLOCK3, d)
            part[:, j:e] = jnp.dot(lhs, w2o[:, j:e], preferred_element_type=F32).astype(BF16)
        d2d_copy(t).start()

        stages(t, ((s2, 1), (s4, 3), (s6, 5)))

    v_copy(in13, early - in13, 1).start()
    s5(n - 5)
    residual(n - 2)
    s1_last(n - 1)
    pl.semaphore_signal(free, inc=1, device_id={"tp": partner}, device_id_type=MESH)
    s6(n - 5)
    v_copy(n - 5, 1, 2).start()
    s3(n - 2)
    s2_last(n - 1)
    residual(n - 1)
    s4(n - 2)
    s4(n - 3)
    s5(n - 4)
    s3_last(n - 1)
    s6(n - 4)
    v_copy(n - 4, 1, 3).start()
    s5(n - 3)
    s5(n - 2)
    s4_last(n - 1)
    s6(n - 3)
    v_copy(n - 3, 1, 4).start()
    s6(n - 2)
    v_copy(n - 2, 1, 5).start()
    s5_last(n - 1)
    got(gr.at[3], chips)
    sent(gs.at[3], chips)
    v_copy(0, in13, 0).wait()
    v_copy(in13, early - in13, 1).wait()
    for i, j in enumerate(range(n - 5, n - 1)):
        v_copy(j, 1, 2 + i).wait()


def finish(n, wbuf, out, sem):
    stores = [pltpu.make_async_copy(wbuf.at[pl.ds(j * TOK, TOK)], out.at[pl.ds(j * TOK, TOK)], sem.at[j]) for j in range(n)]
    for cpy in stores:
        cpy.start()
    for cpy in stores:
        cpy.wait()


def solution(mesh):
    n_tp = mesh.shape["tp"]

    def local(x, gamma, beta, wq, wkv, wo, w1, w3, w2):
        b, s, d = x.shape
        dq, dh, ff = wq.shape[1], wkv.shape[1] // 2, w1.shape[1]
        n = b * s // TOK
        half = TOK // 2
        blk = half // (n_tp // 2)
        assert 2 * ff == d and d // TOK <= n - 6 and d + dq + ff + TOK == n * TOK and n_tp == 8
        dma = pltpu.SemaphoreType.DMA
        hbm = pl.BlockSpec(memory_space=pl.ANY)
        vmem = pl.BlockSpec(memory_space=pltpu.VMEM)
        _, wbuf = pl.pallas_call(
            functools.partial(kernel, n_tp, s),
            out_shape=(jax.ShapeDtypeStruct((b * s, d), BF16), pltpu.VMEM((d + dq + ff + TOK, d), BF16)),
            in_specs=[hbm, vmem, vmem] + [hbm] * 6,
            out_specs=(hbm, vmem),
            scratch_shapes=[
                pltpu.VMEM((2, d), F32),
                pltpu.VMEM((d, dq + dh), BF16),
                pltpu.VMEM((half, d), BF16),
                pltpu.VMEM((half, d), BF16),
                pltpu.VMEM((TOK, d), BF16),
                pltpu.VMEM((2, s, dh), BF16),
                pltpu.VMEM((TOK, dq + ff), BF16),
                pltpu.VMEM((3, half, d), BF16),
                pltpu.VMEM((3, blk, d), BF16),
                pltpu.VMEM((3, 2, blk, d), BF16),
                pltpu.VMEM((blk, d), BF16),
                dma((8,)), dma, dma, dma, dma, pltpu.SemaphoreType.REGULAR, dma, dma,
                dma((3,)), dma((3,)), dma((3,)), dma((3,)), dma((3,)),
                dma, dma((4,)), dma((3,)), dma((3,)), dma((4,)), dma((4,)), dma((6,)),
            ],
            compiler_params=pltpu.CompilerParams(collective_id=0, has_side_effects=True, vmem_limit_bytes=VMEM_LIMIT),
        )(x.reshape(b * s, d), gamma, beta, wq, wkv, wo, w1, w3, w2)
        out = pl.pallas_call(
            functools.partial(finish, n),
            out_shape=jax.ShapeDtypeStruct((b * s, d), BF16),
            in_specs=[vmem],
            out_specs=hbm,
            scratch_shapes=[dma((n,))],
            compiler_params=pltpu.CompilerParams(vmem_limit_bytes=8 * 1024 * 1024),
        )(wbuf)
        return out.reshape(b, s, d)

    return jax.shard_map(local, mesh=mesh,
                         in_specs=(P('dp', None, None), P(), P(), P(None, 'tp'), P(), P('tp', None),
                                   P(None, 'tp'), P(None, 'tp'), P('tp', None)),
                         out_specs=P('dp', None, None), check_vma=False)
```
